512 devices in a mesh: row: 16 (over x_hi, y), col: 32 (over z, x_lo, core).
Axes of the slice: x: 4 (x_hi: 2, x_lo: 2; x = x_hi * 2 + x_lo), y: 8, z: 8, core: 2. Of those that a mesh axis runs over, the one named last changes fastest.
Arguments:
- pair_window: bfloat16 [32, 64, 32, 128], P('col', 'row'), may hold values from -6 to 6
- tri_cotangent: bfloat16 [32, 64, 2048, 128], P(None, 'row', 'col'), may hold values from -0.25 to 0.25
- saved_left: bfloat16 [32, 64, 32, 128], P('col', 'row'), may hold values from -6 to 6
- saved_right: bfloat16 [32, 64, 32, 128], P('col', 'row'), may hold values from -6 to 6
- norm_gain: float32 [128], replicated, may hold values from 0.5 to 1.5
- norm_bias: float32 [128], replicated, may hold values from -3 to 3
- proj_weight: bfloat16 [4, 128, 128], replicated, may hold values from -0.5 to 0.5
Outputs:
- pair_grad: bfloat16 [32, 64, 32, 128], P('col', 'row')
- weight_grad: float32 [4, 128, 128], replicated
- norm_grad: float32 [2, 128], replicated
The draws below stay inside these ranges and needn't reach their ends.
All inputs are finite; a program needn't handle non-finite values.
Results may differ from the reference program's by a relative error of at most 0.0085.
Values may be sent and summed in bfloat16 or wider, within the bound.
No kernel may reach another device: no remote copies, remote signals or barrier semaphores. Data moves between devices by JAX's collectives and lax.ppermute only.
A program may use at most 64 MiB of HBM per device.

```python
import jax
import jax.numpy as jnp
from jax import lax

C = 128
H = 128
K = 32
N_TOK = 2048
BLOCKS = 32
TOK_BLOCK = 64


def raised(result, own_key, source, target, shards_of, factor):
    def block_of(position):
        return (jnp.arange(result.shape[position]) // (result.shape[position] // shards_of)).reshape((-1,) + (1,) * (result.ndim - 1 - position))

    near = jax.random.permutation(own_key, shards_of)[block_of(target)]
    far = (block_of(target) + shards_of // 2) % shards_of
    return jnp.where((block_of(source) == near) | (block_of(source) == far), factor * result, result)


def level_of(rng, extent, pieces, least, high):
    factor_of, own = 1.0, jax.random.fold_in(rng, 6)
    for dim, shards_of in pieces:
        draws = jnp.exp(jax.random.uniform(jax.random.fold_in(own, dim), (shards_of,), jnp.float32, least / len(pieces), high / len(pieces)))
        factor_of = factor_of * jnp.repeat(draws, extent[dim] // shards_of).reshape([-1 if axis == dim else 1 for axis in range(len(extent))])
    return factor_of


def normal_values(rng, extent, spread, limit, split=(), dtype=jnp.bfloat16):
    loudness = level_of(rng, extent, split, -0.22, 0.18) if split else 1.0
    values = jax.random.normal(rng, extent, jnp.float32) * spread * loudness
    return jnp.minimum(jnp.maximum(values, -limit), limit).astype(dtype)


def gaussian_with(key, extent, width, most, split, heavy, held_as=jnp.bfloat16):
    drawn = width * jax.random.normal(key, extent, jnp.float32)
    if split:
        drawn = drawn * level_of(key, extent, split, -0.22, 0.18)
    return jnp.clip(raised(drawn, jax.random.fold_in(key, 3), *heavy), -most, most).astype(held_as)


def setup_inputs(seed: int = 0) -> dict:
    arg_keys = jax.random.split(jax.random.key(seed), 8)
    pair_window = normal_values(arg_keys[0], (BLOCKS, TOK_BLOCK, K, C), 1.0, 6.0, ((0, 32), (1, 16)))
    tri_cotangent = gaussian_with(arg_keys[1], (BLOCKS, TOK_BLOCK, N_TOK, H), N_TOK ** -0.5, 0.25, ((1, 16), (2, 32)), (2, 0, 32, 2.75))
    saved_left = normal_values(arg_keys[2], (BLOCKS, TOK_BLOCK, K, H), 1.0, 6.0, ((0, 32), (1, 16)))
    saved_right = normal_values(arg_keys[3], (BLOCKS, TOK_BLOCK, K, H), 1.0, 6.0, ((0, 32), (1, 16)))
    norm_gain = jnp.clip(1.0 + 0.1 * jax.random.normal(arg_keys[4], (C,), jnp.float32), 0.5, 1.5)
    norm_bias = normal_values(arg_keys[5], (C,), 0.5, 3.0, (), jnp.float32)
    proj_weight = normal_values(arg_keys[6], (4, C, H), C ** -0.5, 0.5)
    return {"pair_window": pair_window, "tri_cotangent": tri_cotangent, "saved_left": saved_left, "saved_right": saved_right, "norm_gain": norm_gain, "norm_bias": norm_bias, "proj_weight": proj_weight}


def gated_norm_back(pair_rows, left_grad, right_grad, norm_gain, norm_bias, proj_weight):
    pair = pair_rows.astype(jnp.float32)
    average = lax.optimization_barrier(jnp.mean(pair, axis=-1, keepdims=True))
    centred = pair - average
    variance = lax.optimization_barrier(jnp.mean(centred * centred, axis=-1, keepdims=True))
    inv_std = lax.rsqrt(variance + 1e-05)
    unit_pair = centred * inv_std
    normed = (unit_pair * norm_gain + norm_bias).astype(jnp.bfloat16)
    chans = proj_weight.shape[2]
    stacked = jnp.transpose(proj_weight, (1, 0, 2)).reshape(proj_weight.shape[1], 4 * chans)
    preact = jnp.dot(normed, stacked, preferred_element_type=jnp.float32)
    gate_left = jax.nn.sigmoid(preact[:, :chans])
    value_left = preact[:, chans:2 * chans]
    gate_right = jax.nn.sigmoid(preact[:, 2 * chans:3 * chans])
    value_right = preact[:, 3 * chans:]
    pre_grads = jnp.concatenate([left_grad * value_left * gate_left * (1.0 - gate_left), left_grad * gate_left, right_grad * value_right * gate_right * (1.0 - gate_right), right_grad * gate_right], axis=1).astype(jnp.bfloat16)
    weight_part = lax.dot_general(normed, pre_grads, (((0,), (0,)), ((), ())), preferred_element_type=jnp.float32)
    weight_part = jnp.transpose(weight_part.reshape(proj_weight.shape[1], 4, chans), (1, 0, 2))
    normed_grad = jnp.dot(pre_grads, stacked.T, preferred_element_type=jnp.float32)
    norm_part = jnp.stack([lax.optimization_barrier(jnp.sum(normed_grad * unit_pair, axis=0)), lax.optimization_barrier(jnp.sum(normed_grad, axis=0))])
    scaled_grad = normed_grad * norm_gain
    pair_grad = inv_std * (scaled_grad - lax.optimization_barrier(jnp.mean(scaled_grad, axis=-1, keepdims=True)) - unit_pair * lax.optimization_barrier(jnp.mean(scaled_grad * unit_pair, axis=-1, keepdims=True)))
    return (pair_grad.astype(jnp.bfloat16), weight_part, norm_part)

def reference(pair_window, tri_cotangent, saved_left, saved_right, norm_gain, norm_bias, proj_weight):
    cotangent = tri_cotangent.reshape(N_TOK, N_TOK, H).astype(jnp.float32)
    left = saved_left.reshape(N_TOK, K, H).astype(jnp.float32)
    right = saved_right.reshape(N_TOK, K, H).astype(jnp.float32)
    left_grad = jnp.einsum('ijh,jkh->ikh', cotangent, right)
    right_grad = jnp.einsum('ijh,ikh->jkh', cotangent, left)
    pair_grad, weight_grad, norm_grad = gated_norm_back(pair_window.reshape(N_TOK * K, C), left_grad.reshape(N_TOK * K, H), right_grad.reshape(N_TOK * K, H), norm_gain, norm_bias, proj_weight)
    return (pair_grad.reshape(BLOCKS, TOK_BLOCK, K, C), weight_grad, norm_grad)
```

```python
import jax
import jax.numpy as jnp
from jax import lax
from jax.sharding import PartitionSpec as P


def sent_to_all(x, axis):
    devices = lax.axis_size(axis)
    return lax.all_to_all(jnp.broadcast_to(x[None], (devices, *x.shape)), axis, 0, 0, tiled=True)


def laid_out(parts, dim):
    parts = jnp.moveaxis(parts, 0, dim)
    lengths = parts.shape
    return parts.reshape(*lengths[:dim], lengths[dim] * lengths[dim + 1], *lengths[dim + 2 :])


def collect(x, axis, dim):
    parts = sent_to_all(x, axis)
    return laid_out(parts, dim)


def split_up(x, dim, devices):
    lengths = x.shape
    parts = x.reshape(*lengths[:dim], devices, lengths[dim] // devices, *lengths[dim + 1 :])
    return jnp.moveaxis(parts, dim, 0)


def sent_and_summed(x, axis, dim):
    parts = split_up(x, dim, lax.axis_size(axis))
    arrived = lax.all_to_all(parts, axis, split_axis=0, concat_axis=0, tiled=True)
    return arrived.astype(jnp.float32).sum(axis=0)


def gated_norm_back(pair_rows, left_grad, right_grad, norm_gain, norm_bias, proj_weight):
    pair = pair_rows.astype(jnp.float32)
    average = jnp.mean(pair, axis=-1, keepdims=True)
    centred = pair - average
    variance = jnp.mean(centred * centred, axis=-1, keepdims=True)
    inv_std = lax.rsqrt(variance + 1e-05)
    unit_pair = centred * inv_std
    normed = (unit_pair * norm_gain + norm_bias).astype(jnp.bfloat16)
    chans = proj_weight.shape[2]
    stacked = jnp.transpose(proj_weight, (1, 0, 2)).reshape(proj_weight.shape[1], 4 * chans)
    preact = jnp.dot(normed, stacked, preferred_element_type=jnp.float32)
    gate_left = jax.nn.sigmoid(preact[:, :chans])
    value_left = preact[:, chans : 2 * chans]
    gate_right = jax.nn.sigmoid(preact[:, 2 * chans : 3 * chans])
    value_right = preact[:, 3 * chans :]
    pre_grads = jnp.concatenate(
        [
            left_grad * value_left * gate_left * (1.0 - gate_left),
            left_grad * gate_left,
            right_grad * value_right * gate_right * (1.0 - gate_right),
            right_grad * gate_right,
        ],
        axis=1,
    ).astype(jnp.bfloat16)
    weight_part = lax.dot_general(
        normed, pre_grads, (((0,), (0,)), ((), ())), preferred_element_type=jnp.float32
    )
    weight_part = jnp.transpose(weight_part.reshape(proj_weight.shape[1], 4, chans), (1, 0, 2))
    normed_grad = jnp.dot(pre_grads, stacked.T, preferred_element_type=jnp.float32)
    norm_part = jnp.stack([jnp.sum(normed_grad * unit_pair, axis=0), jnp.sum(normed_grad, axis=0)])
    scaled_grad = normed_grad * norm_gain
    pair_grad = inv_std * (
        scaled_grad
        - jnp.mean(scaled_grad, axis=-1, keepdims=True)
        - unit_pair * jnp.mean(scaled_grad * unit_pair, axis=-1, keepdims=True)
    )
    return (pair_grad.astype(jnp.bfloat16), weight_part, norm_part)


def summed_over_all(weight_part, norm_part):
    cols = lax.axis_size("col")
    shape = weight_part.shape
    width = shape[-1]
    chunks = weight_part.reshape(cols, -1, width)
    rows = chunks.shape[1]
    extra = jnp.zeros((8, width), jnp.float32).at[: norm_part.shape[0]].set(norm_part)
    packed = jnp.concatenate([chunks, jnp.broadcast_to(extra[None], (cols, 8, width))], axis=1)
    arrived = lax.all_to_all(packed, "col", 0, 0, tiled=True)
    part = arrived.sum(axis=0)
    whole = sent_to_all(part, "row").sum(axis=0)
    weight_grad = sent_to_all(whole[:rows], "col").reshape(shape)
    return weight_grad, whole[rows : rows + norm_part.shape[0]]


def on_device(
    pair_window, tri_cotangent, saved_left, saved_right, norm_gain, norm_bias, proj_weight
):
    block_count, own_rows, col_tokens, channels = tri_cotangent.shape
    window_len = saved_left.shape[2]
    right_rows = collect(saved_right, "row", 1)[0]
    cot_flat = tri_cotangent.reshape(block_count * own_rows, col_tokens, channels)
    cot_piece = cot_flat
    left_grad = sent_and_summed(
        jnp.einsum(
            "ijh,jkh->ikh", cot_piece, right_rows, preferred_element_type=jnp.float32
        ).astype(jnp.bfloat16),
        "col",
        0,
    )
    left_rows = collect(saved_left, "col", 0)
    left_flat = left_rows.reshape(block_count * own_rows, window_len, channels)
    cot_piece = cot_flat
    right_grad = sent_and_summed(
        jnp.einsum("ijh,ikh->jkh", cot_piece, left_flat, preferred_element_type=jnp.float32).astype(
            jnp.bfloat16
        ),
        "row",
        0,
    )
    positions = own_rows * window_len
    pair_grad, weight_part, norm_part = gated_norm_back(
        pair_window.reshape(positions, pair_window.shape[3]),
        left_grad.reshape(positions, channels),
        right_grad.reshape(positions, channels),
        norm_gain,
        norm_bias,
        proj_weight,
    )
    weight_grad, norm_grad = summed_over_all(weight_part, norm_part)
    return (pair_grad.reshape(pair_window.shape), weight_grad, norm_grad)


def solution(mesh):
    return jax.shard_map(
        on_device,
        mesh=mesh,
        in_specs=(
            P("col", "row", None, None),
            P(None, "row", "col", None),
            P("col", "row", None, None),
            P("col", "row", None, None),
            P(),
            P(),
            P(),
        ),
        out_specs=(P("col", "row", None, None), P(), P()),
        check_vma=False,
    )
```

```python
import jax
import jax.numpy as jnp
from jax import lax
from jax.sharding import PartitionSpec as P


def sent_to_all(x, axis):
    devices = lax.axis_size(axis)
    return lax.all_to_all(jnp.broadcast_to(x[None], (devices, *x.shape)), axis, 0, 0, tiled=True)


def laid_out(parts, dim):
    parts = jnp.moveaxis(parts, 0, dim)
    lengths = parts.shape
    return parts.reshape(*lengths[:dim], lengths[dim] * lengths[dim + 1], *lengths[dim + 2 :])


def collect(x, axis, dim):
    parts = sent_to_all(x, axis)
    return laid_out(parts, dim)


def split_up(x, dim, devices):
    lengths = x.shape
    parts = x.reshape(*lengths[:dim], devices, lengths[dim] // devices, *lengths[dim + 1 :])
    return jnp.moveaxis(parts, dim, 0)


def sent_and_summed(x, axis, dim):
    parts = split_up(x, dim, lax.axis_size(axis))
    arrived = lax.all_to_all(parts, axis, split_axis=0, concat_axis=0, tiled=True)
    return arrived.astype(jnp.float32).sum(axis=0)


def gated_norm_back(pair_rows, left_grad, right_grad, norm_gain, norm_bias, proj_weight):
    pair = pair_rows.astype(jnp.float32)
    average = jnp.mean(pair, axis=-1, keepdims=True)
    centred = pair - average
    variance = jnp.mean(centred * centred, axis=-1, keepdims=True)
    inv_std = lax.rsqrt(variance + 1e-05)
    unit_pair = centred * inv_std
    normed = (unit_pair * norm_gain + norm_bias).astype(jnp.bfloat16)
    chans = proj_weight.shape[2]
    stacked = jnp.transpose(proj_weight, (1, 0, 2)).reshape(proj_weight.shape[1], 4 * chans)
    preact = jnp.dot(normed, stacked, preferred_element_type=jnp.float32)
    gate_left = jax.nn.sigmoid(preact[:, :chans])
    value_left = preact[:, chans : 2 * chans]
    gate_right = jax.nn.sigmoid(preact[:, 2 * chans : 3 * chans])
    value_right = preact[:, 3 * chans :]
    pre_grads = jnp.concatenate(
        [
            left_grad * value_left * gate_left * (1.0 - gate_left),
            left_grad * gate_left,
            right_grad * value_right * gate_right * (1.0 - gate_right),
            right_grad * gate_right,
        ],
        axis=1,
    ).astype(jnp.bfloat16)
    weight_part = lax.dot_general(
        normed, pre_grads, (((0,), (0,)), ((), ())), preferred_element_type=jnp.float32
    )
    weight_part = jnp.transpose(weight_part.reshape(proj_weight.shape[1], 4, chans), (1, 0, 2))
    normed_grad = jnp.dot(pre_grads, stacked.T, preferred_element_type=jnp.float32)
    norm_part = jnp.stack([jnp.sum(normed_grad * unit_pair, axis=0), jnp.sum(normed_grad, axis=0)])
    scaled_grad = normed_grad * norm_gain
    pair_grad = inv_std * (
        scaled_grad
        - jnp.mean(scaled_grad, axis=-1, keepdims=True)
        - unit_pair * jnp.mean(scaled_grad * unit_pair, axis=-1, keepdims=True)
    )
    return (pair_grad.astype(jnp.bfloat16), weight_part, norm_part)


def summed_over_all(weight_part, norm_part):
    cols = lax.axis_size("col")
    shape = weight_part.shape
    width = shape[-1]
    chunks = weight_part.reshape(cols, -1, width)
    rows = chunks.shape[1]
    extra = jnp.zeros((8, width), jnp.float32).at[: norm_part.shape[0]].set(norm_part)
    packed = jnp.concatenate([chunks, jnp.broadcast_to(extra[None], (cols, 8, width))], axis=1)
    arrived = lax.all_to_all(packed, "col", 0, 0, tiled=True)
    part = arrived.sum(axis=0)
    whole = sent_to_all(part, "row").sum(axis=0)
    weight_grad = sent_to_all(whole[:rows], "col").reshape(shape)
    return weight_grad, whole[rows : rows + norm_part.shape[0]]


def siblings(devices):
    return [[c for c in range(devices) if c % 2 == core] for core in range(2)]


def swapped(x, axis):
    devices = lax.axis_size(axis)
    return lax.ppermute(x, axis, [(c, c ^ 1) for c in range(devices)])


def all_steps(
    pair_window, tri_cotangent, saved_left, saved_right, norm_gain, norm_bias, proj_weight
):
    block_count, own_rows, col_tokens, channels = tri_cotangent.shape
    window_len = saved_left.shape[2]
    cols = lax.axis_size("col")
    half = cols // 2
    core = lax.rem(lax.axis_index("col"), 2)
    groups = siblings(cols)
    right_rows = collect(saved_right, "row", 1)[0]
    cot_flat = jnp.swapaxes(
        tri_cotangent.reshape(half, 2, own_rows, col_tokens, channels), 0, 1
    ).reshape(block_count * own_rows, col_tokens, channels)
    near = jnp.broadcast_to(saved_left, (half, *saved_left.shape[1:]))
    near = lax.all_to_all(near, "col", 0, 0, tiled=True, axis_index_groups=groups)
    left_part = jnp.einsum(
        "ijh,jkh->ikh", cot_flat, right_rows, preferred_element_type=jnp.float32
    ).astype(jnp.bfloat16)
    pairs = left_part.reshape(2, half, own_rows, window_len, channels)
    kept = lax.dynamic_index_in_dim(pairs, core, 0, keepdims=False)
    away = lax.dynamic_index_in_dim(pairs, 1 - core, 0, keepdims=False)
    came = swapped(away, "col")
    chip_part = (kept.astype(jnp.float32) + came.astype(jnp.float32)).astype(jnp.bfloat16)
    left_arrived = lax.all_to_all(chip_part, "col", 0, 0, tiled=True, axis_index_groups=groups)
    far = swapped(near, "col")
    even = jnp.where(core == 0, near, far)
    odd = jnp.where(core == 0, far, near)
    left_flat = jnp.stack([even, odd]).reshape(
        block_count * own_rows, window_len, channels
    )
    right_part = jnp.einsum(
        "ijh,ikh->jkh", cot_flat, left_flat, preferred_element_type=jnp.float32
    ).astype(jnp.bfloat16)
    left_grad = left_arrived.astype(jnp.float32).sum(axis=0)
    right_grad = sent_and_summed(right_part, "row", 0)
    positions = own_rows * window_len
    pair_grad, weight_part, norm_part = gated_norm_back(
        pair_window.reshape(positions, pair_window.shape[3]),
        left_grad.reshape(positions, channels),
        right_grad.reshape(positions, channels),
        norm_gain,
        norm_bias,
        proj_weight,
    )
    weight_grad, norm_grad = summed_over_all(weight_part, norm_part)
    return (pair_grad.reshape(pair_window.shape), weight_grad, norm_grad)


def solution(mesh):
    return jax.shard_map(
        all_steps,
        mesh=mesh,
        in_specs=(
            P("col", "row", None, None),
            P(None, "row", "col", None),
            P("col", "row", None, None),
            P("col", "row", None, None),
            P(),
            P(),
            P(),
        ),
        out_specs=(P("col", "row", None, None), P(), P()),
        check_vma=False,
    )
```

```python
import jax
import jax.numpy as jnp
from jax import lax
from jax.sharding import PartitionSpec as P


def sent_to_all(x, axis):
    devices = lax.axis_size(axis)
    return lax.all_to_all(jnp.broadcast_to(x[None], (devices, *x.shape)), axis, 0, 0, tiled=True)


def laid_out(parts, dim):
    parts = jnp.moveaxis(parts, 0, dim)
    lengths = parts.shape
    return parts.reshape(*lengths[:dim], lengths[dim] * lengths[dim + 1], *lengths[dim + 2 :])


def collect(x, axis, dim):
    parts = sent_to_all(x, axis)
    return laid_out(parts, dim)


def split_up(x, dim, devices):
    lengths = x.shape
    parts = x.reshape(*lengths[:dim], devices, lengths[dim] // devices, *lengths[dim + 1 :])
    return jnp.moveaxis(parts, dim, 0)


def sent_and_summed(x, axis, dim):
    parts = split_up(x, dim, lax.axis_size(axis))
    arrived = lax.all_to_all(parts, axis, split_axis=0, concat_axis=0, tiled=True)
    return arrived.astype(jnp.float32).sum(axis=0)


def gated_norm_back(pair_rows, left_grad, right_grad, norm_gain, norm_bias, proj_weight):
    pair = pair_rows.astype(jnp.float32)
    average = jnp.mean(pair, axis=-1, keepdims=True)
    centred = pair - average
    variance = jnp.mean(centred * centred, axis=-1, keepdims=True)
    inv_std = lax.rsqrt(variance + 1e-05)
    unit_pair = centred * inv_std
    normed = (unit_pair * norm_gain + norm_bias).astype(jnp.bfloat16)
    chans = proj_weight.shape[2]
    stacked = jnp.transpose(proj_weight, (1, 0, 2)).reshape(proj_weight.shape[1], 4 * chans)
    preact = jnp.dot(normed, stacked, preferred_element_type=jnp.float32)
    gate_left = jax.nn.sigmoid(preact[:, :chans])
    value_left = preact[:, chans : 2 * chans]
    gate_right = jax.nn.sigmoid(preact[:, 2 * chans : 3 * chans])
    value_right = preact[:, 3 * chans :]
    pre_grads = jnp.concatenate(
        [
            left_grad * value_left * gate_left * (1.0 - gate_left),
            left_grad * gate_left,
            right_grad * value_right * gate_right * (1.0 - gate_right),
            right_grad * gate_right,
        ],
        axis=1,
    ).astype(jnp.bfloat16)
    weight_part = lax.dot_general(
        normed, pre_grads, (((0,), (0,)), ((), ())), preferred_element_type=jnp.float32
    )
    weight_part = jnp.transpose(weight_part.reshape(proj_weight.shape[1], 4, chans), (1, 0, 2))
    normed_grad = jnp.dot(pre_grads, stacked.T, preferred_element_type=jnp.float32)
    norm_part = jnp.stack([jnp.sum(normed_grad * unit_pair, axis=0), jnp.sum(normed_grad, axis=0)])
    scaled_grad = normed_grad * norm_gain
    pair_grad = inv_std * (
        scaled_grad
        - jnp.mean(scaled_grad, axis=-1, keepdims=True)
        - unit_pair * jnp.mean(scaled_grad * unit_pair, axis=-1, keepdims=True)
    )
    return (pair_grad.astype(jnp.bfloat16), weight_part, norm_part)


def summed_over_all(weight_part, norm_part):
    cols = lax.axis_size("col")
    shape = weight_part.shape
    width = shape[-1]
    chunks = weight_part.reshape(cols, -1, width).astype(jnp.bfloat16)
    rows = chunks.shape[1]
    norm_high = lax.reduce_precision(norm_part, 8, 7)
    norm_low = norm_part - norm_high
    extra = jnp.concatenate(
        [norm_high, norm_low, jnp.zeros((4, width), jnp.float32)], axis=0
    ).astype(jnp.bfloat16)
    packed = jnp.concatenate([chunks, jnp.broadcast_to(extra[None], (cols, 8, width))], axis=1)
    arrived = lax.all_to_all(packed, "col", 0, 0, tiled=True)
    part = arrived.astype(jnp.float32).sum(axis=0)
    whole = sent_to_all(part, "row").sum(axis=0)
    norm_grad = whole[rows : rows + 2] + whole[rows + 2 : rows + 4]
    chunk, norm_grad = lax.optimization_barrier((whole[:rows].astype(jnp.bfloat16), norm_grad))
    weight_grad = sent_to_all(chunk, "col").reshape(shape)
    return weight_grad.astype(jnp.float32), norm_grad


def siblings(devices):
    return [[c for c in range(devices) if c % 2 == core] for core in range(2)]


def swapped(x, axis):
    devices = lax.axis_size(axis)
    return lax.ppermute(x, axis, [(c, c ^ 1) for c in range(devices)])


def all_steps(
    pair_window, tri_cotangent, saved_left, saved_right, norm_gain, norm_bias, proj_weight
):
    block_count, own_rows, col_tokens, channels = tri_cotangent.shape
    window_len = saved_left.shape[2]
    cols = lax.axis_size("col")
    half = cols // 2
    core = lax.rem(lax.axis_index("col"), 2)
    groups = siblings(cols)
    right_rows = collect(saved_right, "row", 1)[0]
    cot_flat = tri_cotangent.reshape(block_count * own_rows, col_tokens, channels)
    near = jnp.broadcast_to(saved_left, (half, *saved_left.shape[1:]))
    near = lax.all_to_all(near, "col", 0, 0, tiled=True, axis_index_groups=groups)
    left_part = jnp.einsum(
        "ijh,jkh->ikh", cot_flat, right_rows, preferred_element_type=jnp.float32
    ).astype(jnp.bfloat16)
    pairs = left_part.reshape(half, 2, own_rows, window_len, channels)
    kept = lax.dynamic_index_in_dim(pairs, core, 1, keepdims=False)
    away = lax.dynamic_index_in_dim(pairs, 1 - core, 1, keepdims=False)
    came = swapped(away, "col")
    chip_part = (kept.astype(jnp.float32) + came.astype(jnp.float32)).astype(jnp.bfloat16)
    left_arrived = lax.all_to_all(chip_part, "col", 0, 0, tiled=True, axis_index_groups=groups)
    far = swapped(near, "col")
    mine = jnp.arange(2).reshape(1, 2, 1, 1, 1) == core
    left_flat = jnp.where(mine, near[:, None], far[:, None]).reshape(
        block_count * own_rows, window_len, channels
    )
    right_part = jnp.einsum(
        "ijh,ikh->jkh", cot_flat, left_flat, preferred_element_type=jnp.float32
    ).astype(jnp.bfloat16)
    left_grad = left_arrived.astype(jnp.float32).sum(axis=0)
    right_grad = sent_and_summed(right_part, "row", 0)
    positions = own_rows * window_len
    pair_grad, weight_part, norm_part = gated_norm_back(
        pair_window.reshape(positions, pair_window.shape[3]),
        left_grad.reshape(positions, channels),
        right_grad.reshape(positions, channels),
        norm_gain,
        norm_bias,
        proj_weight,
    )
    pair_grad, weight_part, norm_part = lax.optimization_barrier(
        (pair_grad, weight_part, norm_part)
    )
    weight_grad, norm_grad = summed_over_all(weight_part, norm_part)
    return (pair_grad.reshape(pair_window.shape), weight_grad, norm_grad)


def solution(mesh):
    return jax.shard_map(
        all_steps,
        mesh=mesh,
        in_specs=(
            P("col", "row", None, None),
            P(None, "row", "col", None),
            P("col", "row", None, None),
            P("col", "row", None, None),
            P(),
            P(),
            P(),
        ),
        out_specs=(P("col", "row", None, None), P(), P()),
        check_vma=False,
    )
```

```python
import jax
import jax.numpy as jnp
from jax import lax
from jax.sharding import PartitionSpec as P


def sent_to_all(x, axis):
    devices = lax.axis_size(axis)
    return lax.all_to_all(jnp.broadcast_to(x[None], (devices, *x.shape)), axis, 0, 0, tiled=True)


def split_up(x, dim, devices):
    lengths = x.shape
    parts = x.reshape(*lengths[:dim], devices, lengths[dim] // devices, *lengths[dim + 1 :])
    return jnp.moveaxis(parts, dim, 0)


def sent_and_summed(x, axis, dim):
    parts = split_up(x, dim, lax.axis_size(axis))
    arrived = lax.all_to_all(parts, axis, split_axis=0, concat_axis=0, tiled=True)
    return arrived.astype(jnp.float32).sum(axis=0)


def gated_norm_back(pair_rows, left_grad, right_grad, norm_gain, norm_bias, proj_weight):
    pair = pair_rows.astype(jnp.float32)
    average = jnp.mean(pair, axis=-1, keepdims=True)
    centred = pair - average
    variance = jnp.mean(centred * centred, axis=-1, keepdims=True)
    inv_std = lax.rsqrt(variance + 1e-05)
    unit_pair = centred * inv_std
    normed = (unit_pair * norm_gain + norm_bias).astype(jnp.bfloat16)
    chans = proj_weight.shape[2]
    stacked = jnp.transpose(proj_weight, (1, 0, 2)).reshape(proj_weight.shape[1], 4 * chans)
    preact = jnp.dot(normed, stacked, preferred_element_type=jnp.float32)
    gate_left = jax.nn.sigmoid(preact[:, :chans])
    value_left = preact[:, chans : 2 * chans]
    gate_right = jax.nn.sigmoid(preact[:, 2 * chans : 3 * chans])
    value_right = preact[:, 3 * chans :]
    pre_grads = jnp.concatenate(
        [
            left_grad * value_left * gate_left * (1.0 - gate_left),
            left_grad * gate_left,
            right_grad * value_right * gate_right * (1.0 - gate_right),
            right_grad * gate_right,
        ],
        axis=1,
    ).astype(jnp.bfloat16)
    weight_part = lax.dot_general(
        normed, pre_grads, (((0,), (0,)), ((), ())), preferred_element_type=jnp.float32
    )
    weight_part = jnp.transpose(weight_part.reshape(proj_weight.shape[1], 4, chans), (1, 0, 2))
    normed_grad = jnp.dot(pre_grads, stacked.T, preferred_element_type=jnp.float32)
    norm_part = jnp.stack([jnp.sum(normed_grad * unit_pair, axis=0), jnp.sum(normed_grad, axis=0)])
    scaled_grad = normed_grad * norm_gain
    pair_grad = inv_std * (
        scaled_grad
        - jnp.mean(scaled_grad, axis=-1, keepdims=True)
        - unit_pair * jnp.mean(scaled_grad * unit_pair, axis=-1, keepdims=True)
    )
    return (pair_grad.astype(jnp.bfloat16), weight_part, norm_part)


def summed_over_all(weight_part, norm_part):
    cols = lax.axis_size("col")
    shape = weight_part.shape
    width = shape[-1]
    chunks = weight_part.reshape(cols, -1, width).astype(jnp.bfloat16)
    rows = chunks.shape[1]
    norm_high = lax.reduce_precision(norm_part, 8, 7)
    norm_low = norm_part - norm_high
    extra = jnp.concatenate(
        [norm_high, norm_low, jnp.zeros((4, width), jnp.float32)], axis=0
    ).astype(jnp.bfloat16)
    packed = jnp.concatenate([chunks, jnp.broadcast_to(extra[None], (cols, 8, width))], axis=1)
    arrived = lax.all_to_all(packed, "col", 0, 0, tiled=True)
    part = arrived.astype(jnp.float32).sum(axis=0)
    whole = sent_to_all(part, "row").sum(axis=0)
    norm_grad = whole[rows : rows + 2] + whole[rows + 2 : rows + 4]
    chunk, norm_grad = lax.optimization_barrier((whole[:rows].astype(jnp.bfloat16), norm_grad))
    weight_grad = sent_to_all(chunk, "col").reshape(shape)
    return weight_grad.astype(jnp.float32), norm_grad


def exchanged(x, axis, step):
    devices = lax.axis_size(axis)
    return lax.ppermute(x, axis, [(d, d ^ step) for d in range(devices)])


def with_other(near, far, mine, dim):
    which = jnp.arange(2).reshape([2 if d == dim else 1 for d in range(near.ndim + 1)])
    return jnp.where(which == mine, jnp.expand_dims(near, dim), jnp.expand_dims(far, dim))


def all_steps(
    pair_window, tri_cotangent, saved_left, saved_right, norm_gain, norm_bias, proj_weight
):
    block_count, own_rows, col_tokens, channels = tri_cotangent.shape
    window_len = saved_left.shape[2]
    cols = lax.axis_size("col")
    half = cols // 2
    rows = lax.axis_size("row")
    col, row = lax.axis_index("col"), lax.axis_index("row")
    core, x_low = lax.rem(col, 2), lax.rem(lax.div(col, 2), 2)
    x_high = lax.div(row, rows // 2)
    lines_y = [[x * (rows // 2) + y for y in range(rows // 2)] for x in range(2)]
    lines_z = [[z * 4 + k for z in range(cols // 4)] for k in range(4)]
    one_core = [[c for c in range(cols) if c % 2 == k] for k in range(2)]
    right_near = jnp.broadcast_to(saved_right, (rows // 2, *saved_right.shape[1:]))
    right_near = lax.all_to_all(
        right_near, "row", 0, 0, tiled=True, axis_index_groups=lines_y
    )
    right_far = exchanged(right_near, "row", rows // 2)
    right_rows = with_other(right_near, right_far, x_high, 0).reshape(
        col_tokens, window_len, channels
    )
    cot_flat = tri_cotangent.reshape(block_count * own_rows, col_tokens, channels)
    left_pair = with_other(saved_left[0], exchanged(saved_left[0], "col", 2), x_low, 0)
    near = jnp.broadcast_to(left_pair[None], (cols // 4, *left_pair.shape))
    near = lax.all_to_all(near, "col", 0, 0, tiled=True, axis_index_groups=lines_z)
    near = near.reshape(half, own_rows, window_len, channels)
    left_part = jnp.einsum(
        "ijh,jkh->ikh", cot_flat, right_rows, preferred_element_type=jnp.float32
    ).astype(jnp.bfloat16)
    pairs = left_part.reshape(half, 2, own_rows, window_len, channels)
    kept = lax.dynamic_index_in_dim(pairs, core, 1, keepdims=False)
    away = lax.dynamic_index_in_dim(pairs, 1 - core, 1, keepdims=False)
    came = exchanged(away, "col", 1)
    chip_part = (kept.astype(jnp.float32) + came.astype(jnp.float32)).astype(jnp.bfloat16)
    left_arrived = lax.all_to_all(chip_part, "col", 0, 0, tiled=True, axis_index_groups=one_core)
    far = exchanged(near, "col", 1)
    left_flat = with_other(near, far, core, 1).reshape(block_count * own_rows, window_len, channels)
    right_part = jnp.einsum(
        "ijh,ikh->jkh", cot_flat, left_flat, preferred_element_type=jnp.float32
    ).astype(jnp.bfloat16)
    left_grad = left_arrived.astype(jnp.float32).sum(axis=0)
    right_grad = sent_and_summed(right_part, "row", 0)
    positions = own_rows * window_len
    pair_grad, weight_part, norm_part = gated_norm_back(
        pair_window.reshape(positions, pair_window.shape[3]),
        left_grad.reshape(positions, channels),
        right_grad.reshape(positions, channels),
        norm_gain,
        norm_bias,
        proj_weight,
    )
    pair_grad, weight_part, norm_part = lax.optimization_barrier(
        (pair_grad, weight_part, norm_part)
    )
    weight_grad, norm_grad = summed_over_all(weight_part, norm_part)
    return (pair_grad.reshape(pair_window.shape), weight_grad, norm_grad)


def solution(mesh):
    return jax.shard_map(
        all_steps,
        mesh=mesh,
        in_specs=(
            P("col", "row", None, None),
            P(None, "row", "col", None),
            P("col", "row", None, None),
            P("col", "row", None, None),
            P(),
            P(),
            P(),
        ),
        out_specs=(P("col", "row", None, None), P(), P()),
        check_vma=False,
    )
```

```python
import functools

import jax
import jax.numpy as jnp
from jax import lax
from jax.experimental import pallas as pl
from jax.experimental.pallas import tpu as pltpu
from jax.sharding import PartitionSpec as P


def sent_to_all(x, axis):
    devices = lax.axis_size(axis)
    return lax.all_to_all(jnp.broadcast_to(x[None], (devices, *x.shape)), axis, 0, 0, tiled=True)


def split_up(x, dim, devices):
    lengths = x.shape
    parts = x.reshape(*lengths[:dim], devices, lengths[dim] // devices, *lengths[dim + 1 :])
    return jnp.moveaxis(parts, dim, 0)


def sent_and_summed(x, axis, dim):
    parts = split_up(x, dim, lax.axis_size(axis))
    arrived = lax.all_to_all(parts, axis, split_axis=0, concat_axis=0, tiled=True)
    return arrived.astype(jnp.float32).sum(axis=0)


def gated_norm_back(pair_rows, left_grad, right_grad, norm_gain, norm_bias, proj_weight):
    pair = pair_rows.astype(jnp.float32)
    average = jnp.mean(pair, axis=-1, keepdims=True)
    centred = pair - average
    variance = jnp.mean(centred * centred, axis=-1, keepdims=True)
    inv_std = lax.rsqrt(variance + 1e-05)
    unit_pair = centred * inv_std
    normed = (unit_pair * norm_gain + norm_bias).astype(jnp.bfloat16)
    chans = proj_weight.shape[2]
    stacked = jnp.transpose(proj_weight, (1, 0, 2)).reshape(proj_weight.shape[1], 4 * chans)
    preact = jnp.dot(normed, stacked, preferred_element_type=jnp.float32)
    gate_left = jax.nn.sigmoid(preact[:, :chans])
    value_left = preact[:, chans : 2 * chans]
    gate_right = jax.nn.sigmoid(preact[:, 2 * chans : 3 * chans])
    value_right = preact[:, 3 * chans :]
    pre_grads = jnp.concatenate(
        [
            left_grad * value_left * gate_left * (1.0 - gate_left),
            left_grad * gate_left,
            right_grad * value_right * gate_right * (1.0 - gate_right),
            right_grad * gate_right,
        ],
        axis=1,
    ).astype(jnp.bfloat16)
    weight_part = lax.dot_general(
        normed, pre_grads, (((0,), (0,)), ((), ())), preferred_element_type=jnp.float32
    )
    weight_part = jnp.transpose(weight_part.reshape(proj_weight.shape[1], 4, chans), (1, 0, 2))
    normed_grad = jnp.dot(pre_grads, stacked.T, preferred_element_type=jnp.float32)
    norm_part = jnp.stack([jnp.sum(normed_grad * unit_pair, axis=0), jnp.sum(normed_grad, axis=0)])
    scaled_grad = normed_grad * norm_gain
    pair_grad = inv_std * (
        scaled_grad
        - jnp.mean(scaled_grad, axis=-1, keepdims=True)
        - unit_pair * jnp.mean(scaled_grad * unit_pair, axis=-1, keepdims=True)
    )
    return (pair_grad.astype(jnp.bfloat16), weight_part, norm_part)


def summed_over_all(weight_part, norm_part):
    cols = lax.axis_size("col")
    shape = weight_part.shape
    width = shape[-1]
    chunks = weight_part.reshape(cols, -1, width).astype(jnp.bfloat16)
    rows = chunks.shape[1]
    norm_high = lax.reduce_precision(norm_part, 8, 7)
    norm_low = norm_part - norm_high
    extra = jnp.concatenate(
        [norm_high, norm_low, jnp.zeros((4, width), jnp.float32)], axis=0
    ).astype(jnp.bfloat16)
    packed = jnp.concatenate([chunks, jnp.broadcast_to(extra[None], (cols, 8, width))], axis=1)
    arrived = lax.all_to_all(packed, "col", 0, 0, tiled=True)
    part = arrived.astype(jnp.float32).sum(axis=0)
    whole = sent_to_all(part, "row").sum(axis=0)
    norm_grad = whole[rows : rows + 2] + whole[rows + 2 : rows + 4]
    chunk, norm_grad = lax.optimization_barrier((whole[:rows].astype(jnp.bfloat16), norm_grad))
    weight_grad = sent_to_all(chunk, "col").reshape(shape)
    return weight_grad.astype(jnp.float32), norm_grad


def exchanged(x, axis, step):
    devices = lax.axis_size(axis)
    return lax.ppermute(x, axis, [(d, d ^ step) for d in range(devices)])


def with_other(near, far, mine, dim):
    which = jnp.arange(2).reshape([2 if d == dim else 1 for d in range(near.ndim + 1)])
    return jnp.where(which == mine, jnp.expand_dims(near, dim), jnp.expand_dims(far, dim))


PAD = 8
ROWS_TURNED = (((1,), (1,)), ((), ()))


def turned(x):
    n = x.shape[1]
    eye = lax.broadcasted_iota(jnp.int32, (n, n), 0) == lax.broadcasted_iota(jnp.int32, (n, n), 1)
    return lax.dot_general(
        eye.astype(jnp.float32).astype(jnp.bfloat16),
        x,
        ROWS_TURNED,
        preferred_element_type=jnp.float32,
    )


def left_kernel(window_len, place_ref, near_ref, far_ref, cot_ref, kept_ref, away_ref, *scratch):
    wide, by_key, product, rows_out = scratch
    hidden, cols, rows = cot_ref.shape
    x_high, core = place_ref[0], place_ref[1]
    group, step = window_len + PAD, hidden + PAD
    for source, half in ((near_ref, x_high), (far_ref, 1 - x_high)):
        for j in range(cols // 2):
            at = pl.multiple_of((half * (cols // 2) + j) * group, 8)
            wide[pl.ds(at, window_len), :] = source[pl.ds(j * window_len, window_len), :].astype(
                jnp.float32
            )
    for k in range(window_len):
        by_key[pl.ds(k * step, hidden), :] = turned(
            wide[pl.ds(k, cols, stride=group), :].astype(jnp.bfloat16)
        )
    for h in range(hidden):
        keys = by_key[pl.ds(h, window_len, stride=step), :].astype(jnp.bfloat16)
        product[pl.ds(h, window_len, stride=step), :] = jnp.dot(
            keys, cot_ref[h], preferred_element_type=jnp.float32
        )
    for k in range(window_len):
        rows_out[pl.ds(k, rows, stride=group), :] = turned(
            product[pl.ds(k * step, hidden), :].astype(jnp.bfloat16)
        )
    tokens = kept_ref.shape[1] // window_len
    for target, side in ((kept_ref, core), (away_ref, 1 - core)):
        for q in range(kept_ref.shape[0]):
            for t in range(tokens):
                at = pl.multiple_of(((2 * q + side) * tokens + t) * group, 8)
                target[q, pl.ds(t * window_len, window_len), :] = rows_out[
                    pl.ds(at, window_len), :
                ].astype(jnp.bfloat16)


def left_parts(place, near, far, cot_turned, blocks, window_len):
    hidden, cols, rows = cot_turned.shape
    group, step = window_len + PAD, hidden + PAD
    out = jax.ShapeDtypeStruct((blocks // 2, rows * window_len // blocks, hidden), jnp.bfloat16)
    here = pl.BlockSpec(memory_space=pltpu.VMEM)
    return pl.pallas_call(
        functools.partial(left_kernel, window_len),
        out_shape=(out, out),
        in_specs=[pl.BlockSpec(memory_space=pltpu.SMEM), here, here, here],
        out_specs=(here, here),
        scratch_shapes=[
            pltpu.VMEM((cols * group, hidden), jnp.float32),
            pltpu.VMEM((window_len * step, cols), jnp.float32),
            pltpu.VMEM((window_len * step, rows), jnp.float32),
            pltpu.VMEM((rows * group, hidden), jnp.float32),
        ],
        name="left_parts",
    )(place, near, far, cot_turned)


def right_kernel(window_len, place_ref, near_ref, far_ref, cot_ref, out_ref, *scratch):
    wide, by_key, product, rows_out = scratch
    hidden, cols, rows = cot_ref.shape
    core = place_ref[1]
    group, step = window_len + PAD, hidden + PAD
    tokens = near_ref.shape[1] // window_len
    for source, side in ((near_ref, core), (far_ref, 1 - core)):
        for q in range(near_ref.shape[0]):
            for t in range(tokens):
                at = pl.multiple_of(((2 * q + side) * tokens + t) * group, 8)
                wide[pl.ds(at, window_len), :] = source[
                    q, pl.ds(t * window_len, window_len), :
                ].astype(jnp.float32)
    for k in range(window_len):
        by_key[pl.ds(k * step, hidden), :] = turned(
            wide[pl.ds(k, rows, stride=group), :].astype(jnp.bfloat16)
        )
    for h in range(hidden):
        keys = by_key[pl.ds(h, window_len, stride=step), :].astype(jnp.bfloat16)
        product[pl.ds(h, window_len, stride=step), :] = lax.dot_general(
            keys, cot_ref[h], ROWS_TURNED, preferred_element_type=jnp.float32
        )
    for k in range(window_len):
        rows_out[pl.ds(k, cols, stride=group), :] = turned(
            product[pl.ds(k * step, hidden), :].astype(jnp.bfloat16)
        )
    for j in range(cols):
        out_ref[pl.ds(j * window_len, window_len), :] = rows_out[
            pl.ds(j * group, window_len), :
        ].astype(jnp.bfloat16)


def right_parts(place, near, far, cot_turned, window_len):
    hidden, cols, rows = cot_turned.shape
    group, step = window_len + PAD, hidden + PAD
    here = pl.BlockSpec(memory_space=pltpu.VMEM)
    return pl.pallas_call(
        functools.partial(right_kernel, window_len),
        out_shape=jax.ShapeDtypeStruct((cols * window_len, hidden), jnp.bfloat16),
        in_specs=[pl.BlockSpec(memory_space=pltpu.SMEM), here, here, here],
        out_specs=here,
        scratch_shapes=[
            pltpu.VMEM((rows * group, hidden), jnp.float32),
            pltpu.VMEM((window_len * step, rows), jnp.float32),
            pltpu.VMEM((window_len * step, cols), jnp.float32),
            pltpu.VMEM((cols * group, hidden), jnp.float32),
        ],
        name="right_parts",
    )(place, near, far, cot_turned)


def all_steps(
    pair_window, tri_cotangent, saved_left, saved_right, norm_gain, norm_bias, proj_weight
):
    block_count, own_rows, col_tokens, channels = tri_cotangent.shape
    window_len = saved_left.shape[2]
    cols = lax.axis_size("col")
    half = cols // 2
    rows = lax.axis_size("row")
    col, row = lax.axis_index("col"), lax.axis_index("row")
    core, x_low = lax.rem(col, 2), lax.rem(lax.div(col, 2), 2)
    x_high = lax.div(row, rows // 2)
    lines_y = [[x * (rows // 2) + y for y in range(rows // 2)] for x in range(2)]
    lines_z = [[z * 4 + k for z in range(cols // 4)] for k in range(4)]
    one_core = [[c for c in range(cols) if c % 2 == k] for k in range(2)]
    right_near = jnp.broadcast_to(saved_right, (rows // 2, *saved_right.shape[1:]))
    right_near = lax.all_to_all(
        right_near, "row", 0, 0, tiled=True, axis_index_groups=lines_y
    )
    right_far = exchanged(right_near, "row", rows // 2)
    cot_turned = lax.optimization_barrier(
        jnp.transpose(
            tri_cotangent.reshape(block_count * own_rows, col_tokens, channels), (2, 1, 0)
        )
    )
    place = jnp.stack([x_high, core])
    left_pair = with_other(saved_left[0], exchanged(saved_left[0], "col", 2), x_low, 0)
    near = jnp.broadcast_to(left_pair[None], (cols // 4, *left_pair.shape))
    near = lax.all_to_all(near, "col", 0, 0, tiled=True, axis_index_groups=lines_z)
    near = near.reshape(half, own_rows * window_len, channels)
    flat = (-1, channels)
    kept, away = left_parts(
        place, right_near.reshape(flat), right_far.reshape(flat), cot_turned, cols, window_len
    )
    came = exchanged(away, "col", 1)
    chip_part = (kept.astype(jnp.float32) + came.astype(jnp.float32)).astype(jnp.bfloat16)
    left_arrived = lax.all_to_all(chip_part, "col", 0, 0, tiled=True, axis_index_groups=one_core)
    far = exchanged(near, "col", 1)
    right_part = right_parts(place, near, far, cot_turned, window_len)
    right_part = right_part.reshape(col_tokens, window_len, channels)
    left_grad = left_arrived.astype(jnp.float32).sum(axis=0)
    right_grad = sent_and_summed(right_part, "row", 0)
    positions = own_rows * window_len
    pair_grad, weight_part, norm_part = gated_norm_back(
        pair_window.reshape(positions, pair_window.shape[3]),
        left_grad.reshape(positions, channels),
        right_grad.reshape(positions, channels),
        norm_gain,
        norm_bias,
        proj_weight,
    )
    pair_grad, weight_part, norm_part = lax.optimization_barrier(
        (pair_grad, weight_part, norm_part)
    )
    weight_grad, norm_grad = summed_over_all(weight_part, norm_part)
    return (pair_grad.reshape(pair_window.shape), weight_grad, norm_grad)


def solution(mesh):
    return jax.shard_map(
        all_steps,
        mesh=mesh,
        in_specs=(
            P("col", "row", None, None),
            P(None, "row", "col", None),
            P("col", "row", None, None),
            P("col", "row", None, None),
            P(),
            P(),
            P(),
        ),
        out_specs=(P("col", "row", None, None), P(), P()),
        check_vma=False,
    )
```

```python
import functools

import jax
import jax.numpy as jnp
from jax import lax
from jax.experimental import pallas as pl
from jax.experimental.pallas import tpu as pltpu
from jax.sharding import PartitionSpec as P


def sent_to_all(x, axis):
    devices = lax.axis_size(axis)
    return lax.all_to_all(jnp.broadcast_to(x[None], (devices, *x.shape)), axis, 0, 0, tiled=True)


def split_up(x, dim, devices):
    lengths = x.shape
    parts = x.reshape(*lengths[:dim], devices, lengths[dim] // devices, *lengths[dim + 1 :])
    return jnp.moveaxis(parts, dim, 0)


def sent_and_summed(x, axis, dim):
    parts = split_up(x, dim, lax.axis_size(axis))
    arrived = lax.all_to_all(parts, axis, split_axis=0, concat_axis=0, tiled=True)
    return arrived.astype(jnp.float32).sum(axis=0)


def gated_norm_back(pair_rows, left_grad, right_grad, norm_gain, norm_bias, proj_weight):
    pair = pair_rows.astype(jnp.float32)
    average = jnp.mean(pair, axis=-1, keepdims=True)
    centred = pair - average
    variance = jnp.mean(centred * centred, axis=-1, keepdims=True)
    inv_std = lax.rsqrt(variance + 1e-05)
    unit_pair = centred * inv_std
    normed = (unit_pair * norm_gain + norm_bias).astype(jnp.bfloat16)
    chans = proj_weight.shape[2]
    stacked = jnp.transpose(proj_weight, (1, 0, 2)).reshape(proj_weight.shape[1], 4 * chans)
    preact = jnp.dot(normed, stacked, preferred_element_type=jnp.float32)
    gate_left = jax.nn.sigmoid(preact[:, :chans])
    value_left = preact[:, chans : 2 * chans]
    gate_right = jax.nn.sigmoid(preact[:, 2 * chans : 3 * chans])
    value_right = preact[:, 3 * chans :]
    pre_grads = jnp.concatenate(
        [
            left_grad * value_left * gate_left * (1.0 - gate_left),
            left_grad * gate_left,
            right_grad * value_right * gate_right * (1.0 - gate_right),
            right_grad * gate_right,
        ],
        axis=1,
    ).astype(jnp.bfloat16)
    weight_part = lax.dot_general(
        normed, pre_grads, (((0,), (0,)), ((), ())), preferred_element_type=jnp.float32
    )
    weight_part = jnp.transpose(weight_part.reshape(proj_weight.shape[1], 4, chans), (1, 0, 2))
    normed_grad = jnp.dot(pre_grads, stacked.T, preferred_element_type=jnp.float32)
    norm_part = jnp.stack([jnp.sum(normed_grad * unit_pair, axis=0), jnp.sum(normed_grad, axis=0)])
    scaled_grad = normed_grad * norm_gain
    pair_grad = inv_std * (
        scaled_grad
        - jnp.mean(scaled_grad, axis=-1, keepdims=True)
        - unit_pair * jnp.mean(scaled_grad * unit_pair, axis=-1, keepdims=True)
    )
    return (pair_grad.astype(jnp.bfloat16), weight_part, norm_part)


def summed_over_all(weight_part, norm_part):
    cols = lax.axis_size("col")
    shape = weight_part.shape
    width = shape[-1]
    chunks = weight_part.reshape(cols, -1, width).astype(jnp.bfloat16)
    rows = chunks.shape[1]
    norm_high = lax.reduce_precision(norm_part, 8, 7)
    norm_low = norm_part - norm_high
    extra = jnp.concatenate(
        [norm_high, norm_low, jnp.zeros((4, width), jnp.float32)], axis=0
    ).astype(jnp.bfloat16)
    packed = jnp.concatenate([chunks, jnp.broadcast_to(extra[None], (cols, 8, width))], axis=1)
    arrived = lax.all_to_all(packed, "col", 0, 0, tiled=True)
    part = arrived.astype(jnp.float32).sum(axis=0)
    whole = sent_to_all(part, "row").sum(axis=0)
    norm_grad = whole[rows : rows + 2] + whole[rows + 2 : rows + 4]
    chunk, norm_grad = lax.optimization_barrier((whole[:rows].astype(jnp.bfloat16), norm_grad))
    weight_grad = sent_to_all(chunk, "col").reshape(shape)
    return weight_grad.astype(jnp.float32), norm_grad


def exchanged(x, axis, step):
    devices = lax.axis_size(axis)
    return lax.ppermute(x, axis, [(d, d ^ step) for d in range(devices)])


PAD = 8
ROWS_TURNED = (((1,), (1,)), ((), ()))


def turned(x):
    n = x.shape[1]
    eye = lax.broadcasted_iota(jnp.int32, (n, n), 0) == lax.broadcasted_iota(jnp.int32, (n, n), 1)
    return lax.dot_general(
        eye.astype(jnp.float32).astype(jnp.bfloat16),
        x,
        ROWS_TURNED,
        preferred_element_type=jnp.float32,
    )


def place_of():
    row, col = lax.axis_index("row"), lax.axis_index("col")
    half = lax.axis_size("row") // 2
    return lax.div(row, half), lax.rem(lax.div(col, 2), 2), lax.rem(col, 2)


def left_kernel(window_len, near_ref, far_ref, cot_hbm, kept_ref, away_ref, *scratch):
    wide, by_key, product, rows_out, cot_ref, arrived = scratch
    fetch = pltpu.make_async_copy(cot_hbm, cot_ref, arrived)
    fetch.start()
    hidden, cols, rows = cot_ref.shape
    x_high, _, core = place_of()
    group, step = window_len + PAD, hidden + PAD
    for source, half in ((near_ref, x_high), (far_ref, 1 - x_high)):
        for j in range(cols // 2):
            at = pl.multiple_of((half * (cols // 2) + j) * group, 8)
            wide[pl.ds(at, window_len), :] = source[pl.ds(j * window_len, window_len), :].astype(
                jnp.float32
            )
    for k in range(window_len):
        by_key[pl.ds(k * step, hidden), :] = turned(
            wide[pl.ds(k, cols, stride=group), :].astype(jnp.bfloat16)
        )
    fetch.wait()
    for h in range(hidden):
        keys = by_key[pl.ds(h, window_len, stride=step), :].astype(jnp.bfloat16)
        product[pl.ds(h, window_len, stride=step), :] = jnp.dot(
            keys, cot_ref[h], preferred_element_type=jnp.float32
        )
    for k in range(window_len):
        rows_out[pl.ds(k, rows, stride=group), :] = turned(
            product[pl.ds(k * step, hidden), :].astype(jnp.bfloat16)
        )
    tokens = kept_ref.shape[1] // window_len
    for target, side in ((kept_ref, core), (away_ref, 1 - core)):
        for q in range(kept_ref.shape[0]):
            for t in range(tokens):
                at = pl.multiple_of(((2 * q + side) * tokens + t) * group, 8)
                target[q, pl.ds(t * window_len, window_len), :] = rows_out[
                    pl.ds(at, window_len), :
                ].astype(jnp.bfloat16)


def left_parts(near, far, cot_turned, blocks, window_len):
    hidden, cols, rows = cot_turned.shape
    group, step = window_len + PAD, hidden + PAD
    out = jax.ShapeDtypeStruct((blocks // 2, rows * window_len // blocks, hidden), jnp.bfloat16)
    here = pl.BlockSpec(memory_space=pltpu.VMEM)
    return pl.pallas_call(
        functools.partial(left_kernel, window_len),
        out_shape=(out, out),
        in_specs=[here, here, pl.BlockSpec(memory_space=pl.ANY)],
        out_specs=(here, here),
        scratch_shapes=[
            pltpu.VMEM((cols * group, hidden), jnp.float32),
            pltpu.VMEM((window_len * step, cols), jnp.float32),
            pltpu.VMEM((window_len * step, rows), jnp.float32),
            pltpu.VMEM((rows * group, hidden), jnp.float32),
            pltpu.VMEM(cot_turned.shape, cot_turned.dtype),
            pltpu.SemaphoreType.DMA,
        ],
        name="left_parts",
    )(near, far, cot_turned)


def right_kernel(window_len, own_ref, x_ref, core_ref, both_ref, cot_hbm, out_ref, *scratch):
    wide, by_key, product, rows_out, cot_ref, arrived = scratch
    fetch = pltpu.make_async_copy(cot_hbm, cot_ref, arrived)
    fetch.start()
    hidden, cols, rows = cot_ref.shape
    _, x_low, core = place_of()
    group, step = window_len + PAD, hidden + PAD
    tokens = own_ref.shape[1] // window_len
    for source, x, side in (
        (own_ref, x_low, core),
        (x_ref, 1 - x_low, core),
        (core_ref, x_low, 1 - core),
        (both_ref, 1 - x_low, 1 - core),
    ):
        for z in range(own_ref.shape[0]):
            for t in range(tokens):
                at = pl.multiple_of(((z * 4 + 2 * x + side) * tokens + t) * group, 8)
                wide[pl.ds(at, window_len), :] = source[
                    z, pl.ds(t * window_len, window_len), :
                ].astype(jnp.float32)
    for k in range(window_len):
        by_key[pl.ds(k * step, hidden), :] = turned(
            wide[pl.ds(k, rows, stride=group), :].astype(jnp.bfloat16)
        )
    fetch.wait()
    for h in range(hidden):
        keys = by_key[pl.ds(h, window_len, stride=step), :].astype(jnp.bfloat16)
        product[pl.ds(h, window_len, stride=step), :] = lax.dot_general(
            keys, cot_ref[h], ROWS_TURNED, preferred_element_type=jnp.float32
        )
    for k in range(window_len):
        rows_out[pl.ds(k, cols, stride=group), :] = turned(
            product[pl.ds(k * step, hidden), :].astype(jnp.bfloat16)
        )
    for j in range(cols):
        out_ref[pl.ds(j * window_len, window_len), :] = rows_out[
            pl.ds(j * group, window_len), :
        ].astype(jnp.bfloat16)


def right_parts(pieces, cot_turned, window_len):
    hidden, cols, rows = cot_turned.shape
    group, step = window_len + PAD, hidden + PAD
    here = pl.BlockSpec(memory_space=pltpu.VMEM)
    return pl.pallas_call(
        functools.partial(right_kernel, window_len),
        out_shape=jax.ShapeDtypeStruct((cols * window_len, hidden), jnp.bfloat16),
        in_specs=[here, here, here, here, pl.BlockSpec(memory_space=pl.ANY)],
        out_specs=here,
        scratch_shapes=[
            pltpu.VMEM((rows * group, hidden), jnp.float32),
            pltpu.VMEM((window_len * step, rows), jnp.float32),
            pltpu.VMEM((window_len * step, cols), jnp.float32),
            pltpu.VMEM((cols * group, hidden), jnp.float32),
            pltpu.VMEM(cot_turned.shape, cot_turned.dtype),
            pltpu.SemaphoreType.DMA,
        ],
        name="right_parts",
    )(*pieces, cot_turned)


def all_steps(
    pair_window, tri_cotangent, saved_left, saved_right, norm_gain, norm_bias, proj_weight
):
    block_count, own_rows, col_tokens, channels = tri_cotangent.shape
    window_len = saved_left.shape[2]
    cols = lax.axis_size("col")
    rows = lax.axis_size("row")
    lines_y = [[x * (rows // 2) + y for y in range(rows // 2)] for x in range(2)]
    lines_z = [[z * 4 + k for z in range(cols // 4)] for k in range(4)]
    one_core = [[c for c in range(cols) if c % 2 == k] for k in range(2)]
    right_near = jnp.broadcast_to(saved_right, (rows // 2, *saved_right.shape[1:]))
    right_near = lax.all_to_all(
        right_near, "row", 0, 0, tiled=True, axis_index_groups=lines_y
    )
    right_far = exchanged(right_near, "row", rows // 2)
    cot_turned = lax.optimization_barrier(
        jnp.transpose(
            tri_cotangent.reshape(block_count * own_rows, col_tokens, channels), (2, 1, 0)
        )
    )
    own = jnp.broadcast_to(saved_left, (cols // 4, *saved_left.shape[1:]))
    own = lax.all_to_all(own, "col", 0, 0, tiled=True, axis_index_groups=lines_z)
    own = own.reshape(cols // 4, own_rows * window_len, channels)
    flat = (-1, channels)
    kept, away = left_parts(
        right_near.reshape(flat), right_far.reshape(flat), cot_turned, cols, window_len
    )
    came = exchanged(away, "col", 1)
    chip_part = (kept.astype(jnp.float32) + came.astype(jnp.float32)).astype(jnp.bfloat16)
    left_arrived = lax.all_to_all(chip_part, "col", 0, 0, tiled=True, axis_index_groups=one_core)
    across = exchanged(own, "col", 2)
    own_pair = exchanged(own, "col", 1)
    across_pair = exchanged(across, "col", 1)
    right_part = right_parts((own, across, own_pair, across_pair), cot_turned, window_len)
    right_part = right_part.reshape(col_tokens, window_len, channels)
    left_grad = left_arrived.astype(jnp.float32).sum(axis=0)
    right_grad = sent_and_summed(right_part, "row", 0)
    positions = own_rows * window_len
    pair_grad, weight_part, norm_part = gated_norm_back(
        pair_window.reshape(positions, pair_window.shape[3]),
        left_grad.reshape(positions, channels),
        right_grad.reshape(positions, channels),
        norm_gain,
        norm_bias,
        proj_weight,
    )
    pair_grad, weight_part, norm_part = lax.optimization_barrier(
        (pair_grad, weight_part, norm_part)
    )
    weight_grad, norm_grad = summed_over_all(weight_part, norm_part)
    return (pair_grad.reshape(pair_window.shape), weight_grad, norm_grad)


def solution(mesh):
    return jax.shard_map(
        all_steps,
        mesh=mesh,
        in_specs=(
            P("col", "row", None, None),
            P(None, "row", "col", None),
            P("col", "row", None, None),
            P("col", "row", None, None),
            P(),
            P(),
            P(),
        ),
        out_specs=(P("col", "row", None, None), P(), P()),
        check_vma=False,
    )
```

```python
import functools

import jax
import jax.numpy as jnp
from jax import lax
from jax.experimental import pallas as pl
from jax.experimental.pallas import tpu as pltpu
from jax.sharding import PartitionSpec as P


def sent_to_all(x, axis):
    devices = lax.axis_size(axis)
    return lax.all_to_all(jnp.broadcast_to(x[None], (devices, *x.shape)), axis, 0, 0, tiled=True)


def split_up(x, dim, devices):
    lengths = x.shape
    parts = x.reshape(*lengths[:dim], devices, lengths[dim] // devices, *lengths[dim + 1 :])
    return jnp.moveaxis(parts, dim, 0)


def sent_and_summed(x, axis, dim):
    parts = split_up(x, dim, lax.axis_size(axis))
    arrived = lax.all_to_all(parts, axis, split_axis=0, concat_axis=0, tiled=True)
    return arrived.astype(jnp.float32).sum(axis=0)


def gated_norm_back(pair_rows, left_grad, right_grad, norm_gain, norm_bias, proj_weight):
    pair = pair_rows.astype(jnp.float32)
    average = jnp.mean(pair, axis=-1, keepdims=True)
    centred = pair - average
    variance = jnp.mean(centred * centred, axis=-1, keepdims=True)
    inv_std = lax.rsqrt(variance + 1e-05)
    unit_pair = centred * inv_std
    normed = (unit_pair * norm_gain + norm_bias).astype(jnp.bfloat16)
    chans = proj_weight.shape[2]
    stacked = jnp.transpose(proj_weight, (1, 0, 2)).reshape(proj_weight.shape[1], 4 * chans)
    preact = jnp.dot(normed, stacked, preferred_element_type=jnp.float32)
    gate_left = jax.nn.sigmoid(preact[:, :chans])
    value_left = preact[:, chans : 2 * chans]
    gate_right = jax.nn.sigmoid(preact[:, 2 * chans : 3 * chans])
    value_right = preact[:, 3 * chans :]
    pre_grads = jnp.concatenate(
        [
            left_grad * value_left * gate_left * (1.0 - gate_left),
            left_grad * gate_left,
            right_grad * value_right * gate_right * (1.0 - gate_right),
            right_grad * gate_right,
        ],
        axis=1,
    ).astype(jnp.bfloat16)
    weight_part = lax.dot_general(
        normed, pre_grads, (((0,), (0,)), ((), ())), preferred_element_type=jnp.float32
    )
    weight_part = jnp.transpose(weight_part.reshape(proj_weight.shape[1], 4, chans), (1, 0, 2))
    normed_grad = jnp.dot(pre_grads, stacked.T, preferred_element_type=jnp.float32)
    norm_part = jnp.stack([jnp.sum(normed_grad * unit_pair, axis=0), jnp.sum(normed_grad, axis=0)])
    scaled_grad = normed_grad * norm_gain
    pair_grad = inv_std * (
        scaled_grad
        - jnp.mean(scaled_grad, axis=-1, keepdims=True)
        - unit_pair * jnp.mean(scaled_grad * unit_pair, axis=-1, keepdims=True)
    )
    return (pair_grad.astype(jnp.bfloat16), weight_part, norm_part)


def summed_over_all(weight_part, norm_part):
    cols = lax.axis_size("col")
    shape = weight_part.shape
    width = shape[-1]
    chunks = weight_part.reshape(cols, -1, width).astype(jnp.bfloat16)
    rows = chunks.shape[1]
    norm_high = lax.reduce_precision(norm_part, 8, 7)
    norm_low = norm_part - norm_high
    extra = jnp.concatenate(
        [norm_high, norm_low, jnp.zeros((4, width), jnp.float32)], axis=0
    ).astype(jnp.bfloat16)
    packed = jnp.concatenate([chunks, jnp.broadcast_to(extra[None], (cols, 8, width))], axis=1)
    arrived = lax.all_to_all(packed, "col", 0, 0, tiled=True)
    part = arrived.astype(jnp.float32).sum(axis=0)
    whole = sent_to_all(part, "row").sum(axis=0)
    norm_grad = whole[rows : rows + 2] + whole[rows + 2 : rows + 4]
    chunk, norm_grad = lax.optimization_barrier((whole[:rows].astype(jnp.bfloat16), norm_grad))
    weight_grad = sent_to_all(chunk, "col").reshape(shape)
    return weight_grad.astype(jnp.float32), norm_grad


def exchanged(x, axis, step):
    devices = lax.axis_size(axis)
    return lax.ppermute(x, axis, [(d, d ^ step) for d in range(devices)])


PAD = 8
VMEM_LIMIT = 24 * 2**20
ROWS_TURNED = (((1,), (1,)), ((), ()))


def turned(x):
    n = x.shape[1]
    eye = lax.broadcasted_iota(jnp.int32, (n, n), 0) == lax.broadcasted_iota(jnp.int32, (n, n), 1)
    return lax.dot_general(
        eye.astype(jnp.float32).astype(jnp.bfloat16),
        x,
        ROWS_TURNED,
        preferred_element_type=jnp.float32,
    )


def place_of():
    row, col = lax.axis_index("row"), lax.axis_index("col")
    half = lax.axis_size("row") // 2
    return lax.div(row, half), lax.rem(lax.div(col, 2), 2), lax.rem(col, 2)


def left_kernel(window_len, near_ref, far_ref, cot_ref, kept_ref, away_ref, *scratch):
    wide, by_key, product, rows_out = scratch
    hidden, cols, rows = cot_ref.shape
    x_high, _, core = place_of()
    group, step = window_len + PAD, hidden + PAD
    for source, half in ((near_ref, x_high), (far_ref, 1 - x_high)):
        for j in range(cols // 2):
            at = pl.multiple_of((half * (cols // 2) + j) * group, 8)
            wide[pl.ds(at, window_len), :] = source[pl.ds(j * window_len, window_len), :].astype(
                jnp.float32
            )
    for k in range(window_len):
        by_key[pl.ds(k * step, hidden), :] = turned(
            wide[pl.ds(k, cols, stride=group), :].astype(jnp.bfloat16)
        )
    for h in range(hidden):
        keys = by_key[pl.ds(h, window_len, stride=step), :].astype(jnp.bfloat16)
        product[pl.ds(h, window_len, stride=step), :] = jnp.dot(
            keys, cot_ref[h], preferred_element_type=jnp.float32
        )
    for k in range(window_len):
        rows_out[pl.ds(k, rows, stride=group), :] = turned(
            product[pl.ds(k * step, hidden), :].astype(jnp.bfloat16)
        )
    tokens = kept_ref.shape[1] // window_len
    for target, side in ((kept_ref, core), (away_ref, 1 - core)):
        for q in range(kept_ref.shape[0]):
            for t in range(tokens):
                at = pl.multiple_of(((2 * q + side) * tokens + t) * group, 8)
                target[q, pl.ds(t * window_len, window_len), :] = rows_out[
                    pl.ds(at, window_len), :
                ].astype(jnp.bfloat16)


def left_parts(near, far, cot_turned, blocks, window_len):
    hidden, cols, rows = cot_turned.shape
    group, step = window_len + PAD, hidden + PAD
    out = jax.ShapeDtypeStruct((blocks // 2, rows * window_len // blocks, hidden), jnp.bfloat16)
    here = pl.BlockSpec(memory_space=pltpu.VMEM)
    return pl.pallas_call(
        functools.partial(left_kernel, window_len),
        out_shape=(out, out),
        in_specs=[here, here, here],
        out_specs=(here, here),
        scratch_shapes=[
            pltpu.VMEM((cols * group, hidden), jnp.float32),
            pltpu.VMEM((window_len * step, cols), jnp.float32),
            pltpu.VMEM((window_len * step, rows), jnp.float32),
            pltpu.VMEM((rows * group, hidden), jnp.float32),
        ],
        compiler_params=pltpu.CompilerParams(vmem_limit_bytes=VMEM_LIMIT),
        name="left_parts",
    )(near, far, cot_turned)


def right_kernel(window_len, own_ref, x_ref, core_ref, both_ref, cot_ref, out_ref, *scratch):
    wide, by_key, product, rows_out = scratch
    hidden, cols, rows = cot_ref.shape
    _, x_low, core = place_of()
    group, step = window_len + PAD, hidden + PAD
    tokens = own_ref.shape[1] // window_len
    for source, x, side in (
        (own_ref, x_low, core),
        (x_ref, 1 - x_low, core),
        (core_ref, x_low, 1 - core),
        (both_ref, 1 - x_low, 1 - core),
    ):
        for z in range(own_ref.shape[0]):
            for t in range(tokens):
                at = pl.multiple_of(((z * 4 + 2 * x + side) * tokens + t) * group, 8)
                wide[pl.ds(at, window_len), :] = source[
                    z, pl.ds(t * window_len, window_len), :
                ].astype(jnp.float32)
    for k in range(window_len):
        by_key[pl.ds(k * step, hidden), :] = turned(
            wide[pl.ds(k, rows, stride=group), :].astype(jnp.bfloat16)
        )
    for h in range(hidden):
        keys = by_key[pl.ds(h, window_len, stride=step), :].astype(jnp.bfloat16)
        product[pl.ds(h, window_len, stride=step), :] = lax.dot_general(
            keys, cot_ref[h], ROWS_TURNED, preferred_element_type=jnp.float32
        )
    for k in range(window_len):
        rows_out[pl.ds(k, cols, stride=group), :] = turned(
            product[pl.ds(k * step, hidden), :].astype(jnp.bfloat16)
        )
    for j in range(cols):
        out_ref[pl.ds(j * window_len, window_len), :] = rows_out[
            pl.ds(j * group, window_len), :
        ].astype(jnp.bfloat16)


def right_parts(pieces, cot_turned, window_len):
    hidden, cols, rows = cot_turned.shape
    group, step = window_len + PAD, hidden + PAD
    here = pl.BlockSpec(memory_space=pltpu.VMEM)
    return pl.pallas_call(
        functools.partial(right_kernel, window_len),
        out_shape=jax.ShapeDtypeStruct((cols * window_len, hidden), jnp.bfloat16),
        in_specs=[here, here, here, here, here],
        out_specs=here,
        scratch_shapes=[
            pltpu.VMEM((rows * group, hidden), jnp.float32),
            pltpu.VMEM((window_len * step, rows), jnp.float32),
            pltpu.VMEM((window_len * step, cols), jnp.float32),
            pltpu.VMEM((cols * group, hidden), jnp.float32),
        ],
        compiler_params=pltpu.CompilerParams(vmem_limit_bytes=VMEM_LIMIT),
        name="right_parts",
    )(*pieces, cot_turned)


def all_steps(
    pair_window, tri_cotangent, saved_left, saved_right, norm_gain, norm_bias, proj_weight
):
    block_count, own_rows, col_tokens, channels = tri_cotangent.shape
    window_len = saved_left.shape[2]
    cols = lax.axis_size("col")
    rows = lax.axis_size("row")
    lines_y = [[x * (rows // 2) + y for y in range(rows // 2)] for x in range(2)]
    lines_z = [[z * 4 + k for z in range(cols // 4)] for k in range(4)]
    one_core = [[c for c in range(cols) if c % 2 == k] for k in range(2)]
    right_near = jnp.broadcast_to(saved_right, (rows // 2, *saved_right.shape[1:]))
    right_near = lax.all_to_all(
        right_near, "row", 0, 0, tiled=True, axis_index_groups=lines_y
    )
    right_far = exchanged(right_near, "row", rows // 2)
    cot_turned = lax.optimization_barrier(
        jnp.transpose(
            tri_cotangent.reshape(block_count * own_rows, col_tokens, channels), (2, 1, 0)
        )
    )
    own = jnp.broadcast_to(saved_left, (cols // 4, *saved_left.shape[1:]))
    own = lax.all_to_all(own, "col", 0, 0, tiled=True, axis_index_groups=lines_z)
    own = own.reshape(cols // 4, own_rows * window_len, channels)
    flat = (-1, channels)
    kept, away = left_parts(
        right_near.reshape(flat), right_far.reshape(flat), cot_turned, cols, window_len
    )
    came = exchanged(away, "col", 1)
    chip_part = (kept.astype(jnp.float32) + came.astype(jnp.float32)).astype(jnp.bfloat16)
    left_arrived = lax.all_to_all(chip_part, "col", 0, 0, tiled=True, axis_index_groups=one_core)
    across = exchanged(own, "col", 2)
    own_pair = exchanged(own, "col", 1)
    across_pair = exchanged(across, "col", 1)
    right_part = right_parts((own, across, own_pair, across_pair), cot_turned, window_len)
    right_part = right_part.reshape(col_tokens, window_len, channels)
    left_grad = left_arrived.astype(jnp.float32).sum(axis=0)
    right_grad = sent_and_summed(right_part, "row", 0)
    positions = own_rows * window_len
    pair_grad, weight_part, norm_part = gated_norm_back(
        pair_window.reshape(positions, pair_window.shape[3]),
        left_grad.reshape(positions, channels),
        right_grad.reshape(positions, channels),
        norm_gain,
        norm_bias,
        proj_weight,
    )
    pair_grad, weight_part, norm_part = lax.optimization_barrier(
        (pair_grad, weight_part, norm_part)
    )
    weight_grad, norm_grad = summed_over_all(weight_part, norm_part)
    return (pair_grad.reshape(pair_window.shape), weight_grad, norm_grad)


def solution(mesh):
    return jax.shard_map(
        all_steps,
        mesh=mesh,
        in_specs=(
            P("col", "row", None, None),
            P(None, "row", "col", None),
            P("col", "row", None, None),
            P("col", "row", None, None),
            P(),
            P(),
            P(),
        ),
        out_specs=(P("col", "row", None, None), P(), P()),
        check_vma=False,
    )
```

```python
import functools

import jax
import jax.numpy as jnp
from jax import lax
from jax.experimental import pallas as pl
from jax.experimental.pallas import tpu as pltpu
from jax.sharding import PartitionSpec as P


def sent_to_all(x, axis):
    devices = lax.axis_size(axis)
    return lax.all_to_all(jnp.broadcast_to(x[None], (devices, *x.shape)), axis, 0, 0, tiled=True)


def split_up(x, dim, devices):
    lengths = x.shape
    parts = x.reshape(*lengths[:dim], devices, lengths[dim] // devices, *lengths[dim + 1 :])
    return jnp.moveaxis(parts, dim, 0)


def sent_and_summed(x, axis, dim):
    parts = split_up(x, dim, lax.axis_size(axis))
    arrived = lax.all_to_all(parts, axis, split_axis=0, concat_axis=0, tiled=True)
    return arrived.astype(jnp.float32).sum(axis=0)


def gated_norm_back(pair_rows, left_grad, right_grad, norm_gain, norm_bias, proj_weight):
    pair = pair_rows.astype(jnp.float32)
    average = jnp.mean(pair, axis=-1, keepdims=True)
    centred = pair - average
    variance = jnp.mean(centred * centred, axis=-1, keepdims=True)
    inv_std = lax.rsqrt(variance + 1e-05)
    unit_pair = centred * inv_std
    normed = (unit_pair * norm_gain + norm_bias).astype(jnp.bfloat16)
    chans = proj_weight.shape[2]
    stacked = jnp.transpose(proj_weight, (1, 0, 2)).reshape(proj_weight.shape[1], 4 * chans)
    preact = jnp.dot(normed, stacked, preferred_element_type=jnp.float32)
    gate_left = jax.nn.sigmoid(preact[:, :chans])
    value_left = preact[:, chans : 2 * chans]
    gate_right = jax.nn.sigmoid(preact[:, 2 * chans : 3 * chans])
    value_right = preact[:, 3 * chans :]
    pre_grads = jnp.concatenate(
        [
            left_grad * value_left * gate_left * (1.0 - gate_left),
            left_grad * gate_left,
            right_grad * value_right * gate_right * (1.0 - gate_right),
            right_grad * gate_right,
        ],
        axis=1,
    ).astype(jnp.bfloat16)
    weight_part = lax.dot_general(
        normed, pre_grads, (((0,), (0,)), ((), ())), preferred_element_type=jnp.float32
    )
    weight_part = jnp.transpose(weight_part.reshape(proj_weight.shape[1], 4, chans), (1, 0, 2))
    normed_grad = jnp.dot(pre_grads, stacked.T, preferred_element_type=jnp.float32)
    norm_part = jnp.stack([jnp.sum(normed_grad * unit_pair, axis=0), jnp.sum(normed_grad, axis=0)])
    scaled_grad = normed_grad * norm_gain
    pair_grad = inv_std * (
        scaled_grad
        - jnp.mean(scaled_grad, axis=-1, keepdims=True)
        - unit_pair * jnp.mean(scaled_grad * unit_pair, axis=-1, keepdims=True)
    )
    return (pair_grad.astype(jnp.bfloat16), weight_part, norm_part)


def with_split_norm(part, rows):
    norm = part[rows : rows + 2] + part[rows + 2 : rows + 4]
    return jnp.concatenate([part[:rows], split_in_two(norm)], axis=0).astype(jnp.bfloat16)


def split_in_two(norm):
    high = lax.reduce_precision(norm, 8, 7)
    return jnp.concatenate([high, norm - high, jnp.zeros((4, norm.shape[1]), norm.dtype)], axis=0)


def summed_over_all(weight_part, norm_part):
    cols = lax.axis_size("col")
    shape = weight_part.shape
    width = shape[-1]
    chunks = weight_part.reshape(cols, -1, width).astype(jnp.bfloat16)
    rows = chunks.shape[1]
    extra = split_in_two(norm_part).astype(jnp.bfloat16)
    packed = jnp.concatenate([chunks, jnp.broadcast_to(extra[None], (cols, 8, width))], axis=1)
    arrived = lax.all_to_all(packed, "col", 0, 0, tiled=True)
    part = arrived.astype(jnp.float32).sum(axis=0)
    whole = sent_to_all(with_split_norm(part, rows), "row").astype(jnp.float32).sum(axis=0)
    norm_grad = whole[rows : rows + 2] + whole[rows + 2 : rows + 4]
    chunk, norm_grad = lax.optimization_barrier((whole[:rows].astype(jnp.bfloat16), norm_grad))
    weight_grad = sent_to_all(chunk, "col").reshape(shape)
    return weight_grad.astype(jnp.float32), norm_grad


def exchanged(x, axis, step):
    devices = lax.axis_size(axis)
    return lax.ppermute(x, axis, [(d, d ^ step) for d in range(devices)])


PAD = 8
VMEM_LIMIT = 24 * 2**20
ROWS_TURNED = (((1,), (1,)), ((), ()))


def turned(x):
    n = x.shape[1]
    eye = lax.broadcasted_iota(jnp.int32, (n, n), 0) == lax.broadcasted_iota(jnp.int32, (n, n), 1)
    return lax.dot_general(
        eye.astype(jnp.float32).astype(jnp.bfloat16),
        x,
        ROWS_TURNED,
        preferred_element_type=jnp.float32,
    )


def place_of():
    row, col = lax.axis_index("row"), lax.axis_index("col")
    half = lax.axis_size("row") // 2
    return lax.div(row, half), lax.rem(lax.div(col, 2), 2), lax.rem(col, 2)


def left_kernel(window_len, near_ref, far_ref, cot_ref, kept_ref, away_ref, *scratch):
    wide, by_key, product, rows_out = scratch
    hidden, cols, rows = cot_ref.shape
    x_high, _, core = place_of()
    group, step = window_len + PAD, hidden + PAD
    for source, half in ((near_ref, x_high), (far_ref, 1 - x_high)):
        for j in range(cols // 2):
            at = pl.multiple_of((half * (cols // 2) + j) * group, 8)
            wide[pl.ds(at, window_len), :] = source[pl.ds(j * window_len, window_len), :].astype(
                jnp.float32
            )
    for k in range(window_len):
        by_key[pl.ds(k * step, hidden), :] = turned(
            wide[pl.ds(k, cols, stride=group), :].astype(jnp.bfloat16)
        )
    for h in range(hidden):
        keys = by_key[pl.ds(h, window_len, stride=step), :].astype(jnp.bfloat16)
        product[pl.ds(h, window_len, stride=step), :] = jnp.dot(
            keys, cot_ref[h], preferred_element_type=jnp.float32
        )
    for k in range(window_len):
        rows_out[pl.ds(k, rows, stride=group), :] = turned(
            product[pl.ds(k * step, hidden), :].astype(jnp.bfloat16)
        )
    tokens = kept_ref.shape[1] // window_len
    for target, side in ((kept_ref, core), (away_ref, 1 - core)):
        for q in range(kept_ref.shape[0]):
            for t in range(tokens):
                at = pl.multiple_of(((2 * q + side) * tokens + t) * group, 8)
                target[q, pl.ds(t * window_len, window_len), :] = rows_out[
                    pl.ds(at, window_len), :
                ].astype(jnp.bfloat16)


def left_parts(near, far, cot_turned, blocks, window_len):
    hidden, cols, rows = cot_turned.shape
    group, step = window_len + PAD, hidden + PAD
    out = jax.ShapeDtypeStruct((blocks // 2, rows * window_len // blocks, hidden), jnp.bfloat16)
    here = pl.BlockSpec(memory_space=pltpu.VMEM)
    return pl.pallas_call(
        functools.partial(left_kernel, window_len),
        out_shape=(out, out),
        in_specs=[here, here, here],
        out_specs=(here, here),
        scratch_shapes=[
            pltpu.VMEM((cols * group, hidden), jnp.float32),
            pltpu.VMEM((window_len * step, cols), jnp.float32),
            pltpu.VMEM((window_len * step, rows), jnp.float32),
            pltpu.VMEM((rows * group, hidden), jnp.float32),
        ],
        compiler_params=pltpu.CompilerParams(vmem_limit_bytes=VMEM_LIMIT),
        name="left_parts",
    )(near, far, cot_turned)


def right_kernel(window_len, own_ref, x_ref, core_ref, both_ref, cot_ref, out_ref, *scratch):
    wide, by_key, product, rows_out = scratch
    hidden, cols, rows = cot_ref.shape
    _, x_low, core = place_of()
    group, step = window_len + PAD, hidden + PAD
    tokens = own_ref.shape[1] // window_len
    for source, x, side in (
        (own_ref, x_low, core),
        (x_ref, 1 - x_low, core),
        (core_ref, x_low, 1 - core),
        (both_ref, 1 - x_low, 1 - core),
    ):
        for z in range(own_ref.shape[0]):
            for t in range(tokens):
                at = pl.multiple_of(((z * 4 + 2 * x + side) * tokens + t) * group, 8)
                wide[pl.ds(at, window_len), :] = source[
                    z, pl.ds(t * window_len, window_len), :
                ].astype(jnp.float32)
    for k in range(window_len):
        by_key[pl.ds(k * step, hidden), :] = turned(
            wide[pl.ds(k, rows, stride=group), :].astype(jnp.bfloat16)
        )
    for h in range(hidden):
        keys = by_key[pl.ds(h, window_len, stride=step), :].astype(jnp.bfloat16)
        product[pl.ds(h, window_len, stride=step), :] = lax.dot_general(
            keys, cot_ref[h], ROWS_TURNED, preferred_element_type=jnp.float32
        )
    for k in range(window_len):
        rows_out[pl.ds(k, cols, stride=group), :] = turned(
            product[pl.ds(k * step, hidden), :].astype(jnp.bfloat16)
        )
    for j in range(cols):
        out_ref[pl.ds(j * window_len, window_len), :] = rows_out[
            pl.ds(j * group, window_len), :
        ].astype(jnp.bfloat16)


def right_parts(pieces, cot_turned, window_len):
    hidden, cols, rows = cot_turned.shape
    group, step = window_len + PAD, hidden + PAD
    here = pl.BlockSpec(memory_space=pltpu.VMEM)
    return pl.pallas_call(
        functools.partial(right_kernel, window_len),
        out_shape=jax.ShapeDtypeStruct((cols * window_len, hidden), jnp.bfloat16),
        in_specs=[here, here, here, here, here],
        out_specs=here,
        scratch_shapes=[
            pltpu.VMEM((rows * group, hidden), jnp.float32),
            pltpu.VMEM((window_len * step, rows), jnp.float32),
            pltpu.VMEM((window_len * step, cols), jnp.float32),
            pltpu.VMEM((cols * group, hidden), jnp.float32),
        ],
        compiler_params=pltpu.CompilerParams(vmem_limit_bytes=VMEM_LIMIT),
        name="right_parts",
    )(*pieces, cot_turned)


def all_steps(
    pair_window, tri_cotangent, saved_left, saved_right, norm_gain, norm_bias, proj_weight
):
    block_count, own_rows, col_tokens, channels = tri_cotangent.shape
    window_len = saved_left.shape[2]
    cols = lax.axis_size("col")
    rows = lax.axis_size("row")
    lines_y = [[x * (rows // 2) + y for y in range(rows // 2)] for x in range(2)]
    lines_z = [[z * 4 + k for z in range(cols // 4)] for k in range(4)]
    one_core = [[c for c in range(cols) if c % 2 == k] for k in range(2)]
    right_near = jnp.broadcast_to(saved_right, (rows // 2, *saved_right.shape[1:]))
    right_near = lax.all_to_all(
        right_near, "row", 0, 0, tiled=True, axis_index_groups=lines_y
    )
    right_far = exchanged(right_near, "row", rows // 2)
    cot_turned = lax.optimization_barrier(
        jnp.transpose(
            tri_cotangent.reshape(block_count * own_rows, col_tokens, channels), (2, 1, 0)
        )
    )
    own = jnp.broadcast_to(saved_left, (cols // 4, *saved_left.shape[1:]))
    own = lax.all_to_all(own, "col", 0, 0, tiled=True, axis_index_groups=lines_z)
    own = own.reshape(cols // 4, own_rows * window_len, channels)
    flat = (-1, channels)
    kept, away = left_parts(
        right_near.reshape(flat), right_far.reshape(flat), cot_turned, cols, window_len
    )
    came = exchanged(away, "col", 1)
    chip_part = (kept.astype(jnp.float32) + came.astype(jnp.float32)).astype(jnp.bfloat16)
    left_arrived = lax.all_to_all(chip_part, "col", 0, 0, tiled=True, axis_index_groups=one_core)
    across = exchanged(own, "col", 2)
    own_pair = exchanged(own, "col", 1)
    across_pair = exchanged(across, "col", 1)
    right_part = right_parts((own, across, own_pair, across_pair), cot_turned, window_len)
    right_part = right_part.reshape(col_tokens, window_len, channels)
    left_grad = left_arrived.astype(jnp.float32).sum(axis=0)
    right_grad = sent_and_summed(right_part, "row", 0)
    positions = own_rows * window_len
    pair_grad, weight_part, norm_part = gated_norm_back(
        pair_window.reshape(positions, pair_window.shape[3]),
        left_grad.reshape(positions, channels),
        right_grad.reshape(positions, channels),
        norm_gain,
        norm_bias,
        proj_weight,
    )
    pair_grad, weight_part, norm_part = lax.optimization_barrier(
        (pair_grad, weight_part, norm_part)
    )
    weight_grad, norm_grad = summed_over_all(weight_part, norm_part)
    return (pair_grad.reshape(pair_window.shape), weight_grad, norm_grad)


def solution(mesh):
    return jax.shard_map(
        all_steps,
        mesh=mesh,
        in_specs=(
            P("col", "row", None, None),
            P(None, "row", "col", None),
            P("col", "row", None, None),
            P("col", "row", None, None),
            P(),
            P(),
            P(),
        ),
        out_specs=(P("col", "row", None, None), P(), P()),
        check_vma=False,
    )
```

```python
import functools

import jax
import jax.numpy as jnp
from jax import lax
from jax.experimental import pallas as pl
from jax.experimental.pallas import tpu as pltpu
from jax.sharding import PartitionSpec as P


def sent_to_all(x, axis):
    devices = lax.axis_size(axis)
    return lax.all_to_all(jnp.broadcast_to(x[None], (devices, *x.shape)), axis, 0, 0, tiled=True)


def split_up(x, dim, devices):
    lengths = x.shape
    parts = x.reshape(*lengths[:dim], devices, lengths[dim] // devices, *lengths[dim + 1 :])
    return jnp.moveaxis(parts, dim, 0)


def sent_and_summed(x, axis, dim):
    parts = split_up(x, dim, lax.axis_size(axis))
    arrived = lax.all_to_all(parts, axis, split_axis=0, concat_axis=0, tiled=True)
    return arrived.astype(jnp.float32).sum(axis=0)


def gated_norm_back(pair_rows, left_grad, right_grad, norm_gain, norm_bias, proj_weight):
    pair = pair_rows.astype(jnp.float32)
    average = jnp.mean(pair, axis=-1, keepdims=True)
    centred = pair - average
    variance = jnp.mean(centred * centred, axis=-1, keepdims=True)
    inv_std = lax.rsqrt(variance + 1e-05)
    unit_pair = centred * inv_std
    normed = (unit_pair * norm_gain + norm_bias).astype(jnp.bfloat16)
    chans = proj_weight.shape[2]
    stacked = jnp.transpose(proj_weight, (1, 0, 2)).reshape(proj_weight.shape[1], 4 * chans)
    preact = jnp.dot(normed, stacked, preferred_element_type=jnp.float32)
    gate_left = jax.nn.sigmoid(preact[:, :chans])
    value_left = preact[:, chans : 2 * chans]
    gate_right = jax.nn.sigmoid(preact[:, 2 * chans : 3 * chans])
    value_right = preact[:, 3 * chans :]
    pre_grads = jnp.concatenate(
        [
            left_grad * value_left * gate_left * (1.0 - gate_left),
            left_grad * gate_left,
            right_grad * value_right * gate_right * (1.0 - gate_right),
            right_grad * gate_right,
        ],
        axis=1,
    ).astype(jnp.bfloat16)
    weight_part = lax.dot_general(
        normed, pre_grads, (((0,), (0,)), ((), ())), preferred_element_type=jnp.float32
    )
    weight_part = jnp.transpose(weight_part.reshape(proj_weight.shape[1], 4, chans), (1, 0, 2))
    normed_grad = jnp.dot(pre_grads, stacked.T, preferred_element_type=jnp.float32)
    norm_part = jnp.stack([jnp.sum(normed_grad * unit_pair, axis=0), jnp.sum(normed_grad, axis=0)])
    scaled_grad = normed_grad * norm_gain
    pair_grad = inv_std * (
        scaled_grad
        - jnp.mean(scaled_grad, axis=-1, keepdims=True)
        - unit_pair * jnp.mean(scaled_grad * unit_pair, axis=-1, keepdims=True)
    )
    return (pair_grad.astype(jnp.bfloat16), weight_part, norm_part)


def with_split_norm(part, rows):
    norm = part[rows : rows + 2] + part[rows + 2 : rows + 4]
    return jnp.concatenate([part[:rows], split_in_two(norm)], axis=0).astype(jnp.bfloat16)


def split_in_two(norm):
    high = lax.reduce_precision(norm, 8, 7)
    return jnp.concatenate([high, norm - high, jnp.zeros((4, norm.shape[1]), norm.dtype)], axis=0)


def summed_over_all(weight_part, norm_part):
    cols = lax.axis_size("col")
    shape = weight_part.shape
    width = shape[-1]
    chunks = weight_part.reshape(cols, -1, width).astype(jnp.bfloat16)
    rows = chunks.shape[1]
    extra = split_in_two(norm_part).astype(jnp.bfloat16)
    packed = jnp.concatenate([chunks, jnp.broadcast_to(extra[None], (cols, 8, width))], axis=1)
    arrived = lax.all_to_all(packed, "col", 0, 0, tiled=True)
    part = arrived.astype(jnp.float32).sum(axis=0)
    whole = sent_to_all(with_split_norm(part, rows), "row").astype(jnp.float32).sum(axis=0)
    norm_grad = whole[rows : rows + 2] + whole[rows + 2 : rows + 4]
    chunk, norm_grad = lax.optimization_barrier((whole[:rows].astype(jnp.bfloat16), norm_grad))
    weight_grad = sent_to_all(chunk, "col").reshape(shape)
    return weight_grad.astype(jnp.float32), norm_grad


def exchanged(x, axis, step):
    devices = lax.axis_size(axis)
    return lax.ppermute(x, axis, [(d, d ^ step) for d in range(devices)])


PAD = 8
VMEM_LIMIT = 24 * 2**20
ROWS_TURNED = (((1,), (1,)), ((), ()))


def turned(x):
    n = x.shape[1]
    eye = lax.broadcasted_iota(jnp.int32, (n, n), 0) == lax.broadcasted_iota(jnp.int32, (n, n), 1)
    return lax.dot_general(
        eye.astype(jnp.float32).astype(jnp.bfloat16),
        x,
        ROWS_TURNED,
        preferred_element_type=jnp.float32,
    )


def place_of():
    col = lax.axis_index("col")
    return lax.rem(lax.div(col, 2), 2), lax.rem(col, 2)


def left_kernel(window_len, rows_ref, cot_ref, kept_ref, away_ref, *scratch):
    wide, by_key, product, rows_out = scratch
    hidden, cols, rows = cot_ref.shape
    _, core = place_of()
    group, step = window_len + PAD, hidden + PAD
    for j in range(cols):
        wide[pl.ds(j * group, window_len), :] = rows_ref[
            pl.ds(j * window_len, window_len), :
        ].astype(jnp.float32)
    for k in range(window_len):
        by_key[pl.ds(k * step, hidden), :] = turned(
            wide[pl.ds(k, cols, stride=group), :].astype(jnp.bfloat16)
        )
    for h in range(hidden):
        keys = by_key[pl.ds(h, window_len, stride=step), :].astype(jnp.bfloat16)
        product[pl.ds(h, window_len, stride=step), :] = jnp.dot(
            keys, cot_ref[h], preferred_element_type=jnp.float32
        )
    for k in range(window_len):
        rows_out[pl.ds(k, rows, stride=group), :] = turned(
            product[pl.ds(k * step, hidden), :].astype(jnp.bfloat16)
        )
    tokens = kept_ref.shape[1] // window_len
    for target, side in ((kept_ref, core), (away_ref, 1 - core)):
        for q in range(kept_ref.shape[0]):
            for t in range(tokens):
                at = pl.multiple_of(((2 * q + side) * tokens + t) * group, 8)
                target[q, pl.ds(t * window_len, window_len), :] = rows_out[
                    pl.ds(at, window_len), :
                ].astype(jnp.bfloat16)


def left_parts(right_rows, cot_turned, blocks, window_len):
    hidden, cols, rows = cot_turned.shape
    group, step = window_len + PAD, hidden + PAD
    out = jax.ShapeDtypeStruct((blocks // 2, rows * window_len // blocks, hidden), jnp.bfloat16)
    here = pl.BlockSpec(memory_space=pltpu.VMEM)
    return pl.pallas_call(
        functools.partial(left_kernel, window_len),
        out_shape=(out, out),
        in_specs=[here, here],
        out_specs=(here, here),
        scratch_shapes=[
            pltpu.VMEM((cols * group, hidden), jnp.float32),
            pltpu.VMEM((window_len * step, cols), jnp.float32),
            pltpu.VMEM((window_len * step, rows), jnp.float32),
            pltpu.VMEM((rows * group, hidden), jnp.float32),
        ],
        compiler_params=pltpu.CompilerParams(vmem_limit_bytes=VMEM_LIMIT),
        name="left_parts",
    )(right_rows, cot_turned)


def right_kernel(window_len, own_ref, x_ref, core_ref, both_ref, cot_ref, out_ref, *scratch):
    wide, by_key, product, rows_out = scratch
    hidden, cols, rows = cot_ref.shape
    x_low, core = place_of()
    group, step = window_len + PAD, hidden + PAD
    tokens = own_ref.shape[1] // window_len
    for source, x, side in (
        (own_ref, x_low, core),
        (x_ref, 1 - x_low, core),
        (core_ref, x_low, 1 - core),
        (both_ref, 1 - x_low, 1 - core),
    ):
        for z in range(own_ref.shape[0]):
            for t in range(tokens):
                at = pl.multiple_of(((z * 4 + 2 * x + side) * tokens + t) * group, 8)
                wide[pl.ds(at, window_len), :] = source[
                    z, pl.ds(t * window_len, window_len), :
                ].astype(jnp.float32)
    for k in range(window_len):
        by_key[pl.ds(k * step, hidden), :] = turned(
            wide[pl.ds(k, rows, stride=group), :].astype(jnp.bfloat16)
        )
    for h in range(hidden):
        keys = by_key[pl.ds(h, window_len, stride=step), :].astype(jnp.bfloat16)
        product[pl.ds(h, window_len, stride=step), :] = lax.dot_general(
            keys, cot_ref[h], ROWS_TURNED, preferred_element_type=jnp.float32
        )
    for k in range(window_len):
        rows_out[pl.ds(k, cols, stride=group), :] = turned(
            product[pl.ds(k * step, hidden), :].astype(jnp.bfloat16)
        )
    for j in range(cols):
        out_ref[pl.ds(j * window_len, window_len), :] = rows_out[
            pl.ds(j * group, window_len), :
        ].astype(jnp.bfloat16)


def right_parts(pieces, cot_turned, window_len):
    hidden, cols, rows = cot_turned.shape
    group, step = window_len + PAD, hidden + PAD
    here = pl.BlockSpec(memory_space=pltpu.VMEM)
    return pl.pallas_call(
        functools.partial(right_kernel, window_len),
        out_shape=jax.ShapeDtypeStruct((cols * window_len, hidden), jnp.bfloat16),
        in_specs=[here, here, here, here, here],
        out_specs=here,
        scratch_shapes=[
            pltpu.VMEM((rows * group, hidden), jnp.float32),
            pltpu.VMEM((window_len * step, rows), jnp.float32),
            pltpu.VMEM((window_len * step, cols), jnp.float32),
            pltpu.VMEM((cols * group, hidden), jnp.float32),
        ],
        compiler_params=pltpu.CompilerParams(vmem_limit_bytes=VMEM_LIMIT),
        name="right_parts",
    )(*pieces, cot_turned)


def all_steps(
    pair_window, tri_cotangent, saved_left, saved_right, norm_gain, norm_bias, proj_weight
):
    block_count, own_rows, col_tokens, channels = tri_cotangent.shape
    window_len = saved_left.shape[2]
    cols = lax.axis_size("col")
    lines_z = [[z * 4 + k for z in range(cols // 4)] for k in range(4)]
    one_core = [[c for c in range(cols) if c % 2 == k] for k in range(2)]
    right_rows = sent_to_all(saved_right[0], "row").reshape(col_tokens * window_len, channels)
    cot_turned = lax.optimization_barrier(
        jnp.transpose(
            tri_cotangent.reshape(block_count * own_rows, col_tokens, channels), (2, 1, 0)
        )
    )
    own = jnp.broadcast_to(saved_left, (cols // 4, *saved_left.shape[1:]))
    own = lax.all_to_all(own, "col", 0, 0, tiled=True, axis_index_groups=lines_z)
    own = own.reshape(cols // 4, own_rows * window_len, channels)
    kept, away = left_parts(right_rows, cot_turned, cols, window_len)
    came = exchanged(away, "col", 1)
    chip_part = (kept.astype(jnp.float32) + came.astype(jnp.float32)).astype(jnp.bfloat16)
    left_arrived = lax.all_to_all(chip_part, "col", 0, 0, tiled=True, axis_index_groups=one_core)
    across = exchanged(own, "col", 2)
    own_pair = exchanged(own, "col", 1)
    across_pair = exchanged(across, "col", 1)
    right_part = right_parts((own, across, own_pair, across_pair), cot_turned, window_len)
    right_part = right_part.reshape(col_tokens, window_len, channels)
    left_grad = left_arrived.astype(jnp.float32).sum(axis=0)
    right_grad = sent_and_summed(right_part, "row", 0)
    positions = own_rows * window_len
    pair_grad, weight_part, norm_part = gated_norm_back(
        pair_window.reshape(positions, pair_window.shape[3]),
        left_grad.reshape(positions, channels),
        right_grad.reshape(positions, channels),
        norm_gain,
        norm_bias,
        proj_weight,
    )
    pair_grad, weight_part, norm_part = lax.optimization_barrier(
        (pair_grad, weight_part, norm_part)
    )
    weight_grad, norm_grad = summed_over_all(weight_part, norm_part)
    return (pair_grad.reshape(pair_window.shape), weight_grad, norm_grad)


def solution(mesh):
    return jax.shard_map(
        all_steps,
        mesh=mesh,
        in_specs=(
            P("col", "row", None, None),
            P(None, "row", "col", None),
            P("col", "row", None, None),
            P("col", "row", None, None),
            P(),
            P(),
            P(),
        ),
        out_specs=(P("col", "row", None, None), P(), P()),
        check_vma=False,
    )
```

```python
import functools

import jax
import jax.numpy as jnp
from jax import lax
from jax.experimental import pallas as pl
from jax.experimental.pallas import tpu as pltpu
from jax.sharding import PartitionSpec as P


def sent_to_all(x, axis):
    devices = lax.axis_size(axis)
    return lax.all_to_all(jnp.broadcast_to(x[None], (devices, *x.shape)), axis, 0, 0, tiled=True)


def split_up(x, dim, devices):
    lengths = x.shape
    parts = x.reshape(*lengths[:dim], devices, lengths[dim] // devices, *lengths[dim + 1 :])
    return jnp.moveaxis(parts, dim, 0)


def sent_and_summed(x, axis, dim):
    parts = split_up(x, dim, lax.axis_size(axis))
    arrived = lax.all_to_all(parts, axis, split_axis=0, concat_axis=0, tiled=True)
    return arrived.astype(jnp.float32).sum(axis=0)


def gated_norm_back(pair_rows, left_grad, right_grad, norm_gain, norm_bias, proj_weight):
    pair = pair_rows.astype(jnp.float32)
    average = jnp.mean(pair, axis=-1, keepdims=True)
    centred = pair - average
    variance = jnp.mean(centred * centred, axis=-1, keepdims=True)
    inv_std = lax.rsqrt(variance + 1e-05)
    unit_pair = centred * inv_std
    normed = (unit_pair * norm_gain + norm_bias).astype(jnp.bfloat16)
    chans = proj_weight.shape[2]
    stacked = jnp.transpose(proj_weight, (1, 0, 2)).reshape(proj_weight.shape[1], 4 * chans)
    preact = jnp.dot(normed, stacked, preferred_element_type=jnp.float32)
    gate_left = jax.nn.sigmoid(preact[:, :chans])
    value_left = preact[:, chans : 2 * chans]
    gate_right = jax.nn.sigmoid(preact[:, 2 * chans : 3 * chans])
    value_right = preact[:, 3 * chans :]
    pre_grads = jnp.concatenate(
        [
            left_grad * value_left * gate_left * (1.0 - gate_left),
            left_grad * gate_left,
            right_grad * value_right * gate_right * (1.0 - gate_right),
            right_grad * gate_right,
        ],
        axis=1,
    ).astype(jnp.bfloat16)
    weight_part = lax.dot_general(
        normed, pre_grads, (((0,), (0,)), ((), ())), preferred_element_type=jnp.float32
    )
    weight_part = jnp.transpose(weight_part.reshape(proj_weight.shape[1], 4, chans), (1, 0, 2))
    normed_grad = jnp.dot(pre_grads, stacked.T, preferred_element_type=jnp.float32)
    norm_part = jnp.stack([jnp.sum(normed_grad * unit_pair, axis=0), jnp.sum(normed_grad, axis=0)])
    scaled_grad = normed_grad * norm_gain
    pair_grad = inv_std * (
        scaled_grad
        - jnp.mean(scaled_grad, axis=-1, keepdims=True)
        - unit_pair * jnp.mean(scaled_grad * unit_pair, axis=-1, keepdims=True)
    )
    return (pair_grad.astype(jnp.bfloat16), weight_part, norm_part)


def with_split_norm(part, rows):
    norm = part[rows : rows + 2] + part[rows + 2 : rows + 4]
    return jnp.concatenate([part[:rows], split_in_two(norm)], axis=0).astype(jnp.bfloat16)


def split_in_two(norm):
    high = lax.reduce_precision(norm, 8, 7)
    return jnp.concatenate([high, norm - high, jnp.zeros((4, norm.shape[1]), norm.dtype)], axis=0)


def summed_over_all(weight_part, norm_part):
    cols = lax.axis_size("col")
    shape = weight_part.shape
    width = shape[-1]
    chunks = weight_part.reshape(cols, -1, width).astype(jnp.bfloat16)
    rows = chunks.shape[1]
    extra = split_in_two(norm_part).astype(jnp.bfloat16)
    packed = jnp.concatenate([chunks, jnp.broadcast_to(extra[None], (cols, 8, width))], axis=1)
    arrived = lax.all_to_all(packed, "col", 0, 0, tiled=True)
    part = arrived.astype(jnp.float32).sum(axis=0)
    whole = sent_to_all(with_split_norm(part, rows), "row").astype(jnp.float32).sum(axis=0)
    chunk, sums = lax.optimization_barrier((whole[:rows].astype(jnp.bfloat16), whole[rows:]))
    weight_grad = sent_to_all(chunk, "col").reshape(-1, width)
    weight_grad, norm_grad = final_sums(weight_grad, sums)
    return weight_grad.reshape(shape), norm_grad


def exchanged(x, axis, step):
    devices = lax.axis_size(axis)
    return lax.ppermute(x, axis, [(d, d ^ step) for d in range(devices)])


PAD = 8
VMEM_LIMIT = 24 * 2**20
ROWS_TURNED = (((1,), (1,)), ((), ()))


def turned(x):
    n = x.shape[1]
    eye = lax.broadcasted_iota(jnp.int32, (n, n), 0) == lax.broadcasted_iota(jnp.int32, (n, n), 1)
    return lax.dot_general(
        eye.astype(jnp.float32).astype(jnp.bfloat16),
        x,
        ROWS_TURNED,
        preferred_element_type=jnp.float32,
    )


def place_of():
    row, col = lax.axis_index("row"), lax.axis_index("col")
    half = lax.axis_size("row") // 2
    return lax.div(row, half), lax.rem(lax.div(col, 2), 2), lax.rem(col, 2)


def left_kernel(window_len, near_ref, far_ref, cot_ref, kept_ref, away_ref, *scratch):
    wide, by_key, product, rows_out = scratch
    hidden, cols, rows = cot_ref.shape
    x_high, _, core = place_of()
    group, step = window_len + PAD, hidden + PAD
    for source, half in ((near_ref, x_high), (far_ref, 1 - x_high)):
        for j in range(cols // 2):
            at = pl.multiple_of((half * (cols // 2) + j) * group, 8)
            wide[pl.ds(at, window_len), :] = source[pl.ds(j * window_len, window_len), :].astype(
                jnp.float32
            )
    for k in range(window_len):
        by_key[pl.ds(k * step, hidden), :] = turned(
            wide[pl.ds(k, cols, stride=group), :].astype(jnp.bfloat16)
        )
    for h in range(hidden):
        keys = by_key[pl.ds(h, window_len, stride=step), :].astype(jnp.bfloat16)
        product[pl.ds(h, window_len, stride=step), :] = jnp.dot(
            keys, cot_ref[h], preferred_element_type=jnp.float32
        )
    for k in range(window_len):
        rows_out[pl.ds(k, rows, stride=group), :] = turned(
            product[pl.ds(k * step, hidden), :].astype(jnp.bfloat16)
        )
    tokens = kept_ref.shape[1] // window_len
    for target, side in ((kept_ref, core), (away_ref, 1 - core)):
        for q in range(kept_ref.shape[0]):
            for t in range(tokens):
                at = pl.multiple_of(((2 * q + side) * tokens + t) * group, 8)
                target[q, pl.ds(t * window_len, window_len), :] = rows_out[
                    pl.ds(at, window_len), :
                ].astype(jnp.bfloat16)


def left_parts(near, far, cot_turned, blocks, window_len):
    hidden, cols, rows = cot_turned.shape
    group, step = window_len + PAD, hidden + PAD
    out = jax.ShapeDtypeStruct((blocks // 2, rows * window_len // blocks, hidden), jnp.bfloat16)
    here = pl.BlockSpec(memory_space=pltpu.VMEM)
    return pl.pallas_call(
        functools.partial(left_kernel, window_len),
        out_shape=(out, out),
        in_specs=[here, here, here],
        out_specs=(here, here),
        scratch_shapes=[
            pltpu.VMEM((cols * group, hidden), jnp.float32),
            pltpu.VMEM((window_len * step, cols), jnp.float32),
            pltpu.VMEM((window_len * step, rows), jnp.float32),
            pltpu.VMEM((rows * group, hidden), jnp.float32),
        ],
        compiler_params=pltpu.CompilerParams(vmem_limit_bytes=VMEM_LIMIT),
        name="left_parts",
    )(near, far, cot_turned)


def right_kernel(window_len, own_ref, x_ref, core_ref, both_ref, cot_ref, out_ref, *scratch):
    wide, by_key, product, rows_out = scratch
    hidden, cols, rows = cot_ref.shape
    _, x_low, core = place_of()
    group, step = window_len + PAD, hidden + PAD
    tokens = own_ref.shape[1] // window_len
    for source, x, side in (
        (own_ref, x_low, core),
        (x_ref, 1 - x_low, core),
        (core_ref, x_low, 1 - core),
        (both_ref, 1 - x_low, 1 - core),
    ):
        for z in range(own_ref.shape[0]):
            for t in range(tokens):
                at = pl.multiple_of(((z * 4 + 2 * x + side) * tokens + t) * group, 8)
                wide[pl.ds(at, window_len), :] = source[
                    z, pl.ds(t * window_len, window_len), :
                ].astype(jnp.float32)
    for k in range(window_len):
        by_key[pl.ds(k * step, hidden), :] = turned(
            wide[pl.ds(k, rows, stride=group), :].astype(jnp.bfloat16)
        )
    for h in range(hidden):
        keys = by_key[pl.ds(h, window_len, stride=step), :].astype(jnp.bfloat16)
        product[pl.ds(h, window_len, stride=step), :] = lax.dot_general(
            keys, cot_ref[h], ROWS_TURNED, preferred_element_type=jnp.float32
        )
    for k in range(window_len):
        rows_out[pl.ds(k, cols, stride=group), :] = turned(
            product[pl.ds(k * step, hidden), :].astype(jnp.bfloat16)
        )
    for j in range(cols):
        out_ref[pl.ds(j * window_len, window_len), :] = rows_out[
            pl.ds(j * group, window_len), :
        ].astype(jnp.bfloat16)


def right_parts(pieces, cot_turned, window_len):
    hidden, cols, rows = cot_turned.shape
    group, step = window_len + PAD, hidden + PAD
    here = pl.BlockSpec(memory_space=pltpu.VMEM)
    return pl.pallas_call(
        functools.partial(right_kernel, window_len),
        out_shape=jax.ShapeDtypeStruct((cols * window_len, hidden), jnp.bfloat16),
        in_specs=[here, here, here, here, here],
        out_specs=here,
        scratch_shapes=[
            pltpu.VMEM((rows * group, hidden), jnp.float32),
            pltpu.VMEM((window_len * step, rows), jnp.float32),
            pltpu.VMEM((window_len * step, cols), jnp.float32),
            pltpu.VMEM((cols * group, hidden), jnp.float32),
        ],
        compiler_params=pltpu.CompilerParams(vmem_limit_bytes=VMEM_LIMIT),
        name="right_parts",
    )(*pieces, cot_turned)


def pair_kernel(kept_ref, came_ref, out_ref):
    total = kept_ref[...].astype(jnp.float32) + came_ref[...].astype(jnp.float32)
    out_ref[...] = total.astype(jnp.bfloat16)


def pair_sum(kept, came):
    here = pl.BlockSpec(memory_space=pltpu.VMEM)
    return pl.pallas_call(
        pair_kernel,
        out_shape=jax.ShapeDtypeStruct(kept.shape, kept.dtype),
        in_specs=[here, here],
        out_specs=here,
        compiler_params=pltpu.CompilerParams(vmem_limit_bytes=VMEM_LIMIT // 4),
        name="pair_sum",
    )(kept, came)


def final_kernel(weight_ref, sums_ref, weight_out, norm_out):
    weight_out[...] = weight_ref[...].astype(jnp.float32)
    norm_out[...] = sums_ref[0:2, :] + sums_ref[2:4, :]


def final_sums(weight, sums):
    here = pl.BlockSpec(memory_space=pltpu.VMEM)
    return pl.pallas_call(
        final_kernel,
        out_shape=(
            jax.ShapeDtypeStruct(weight.shape, jnp.float32),
            jax.ShapeDtypeStruct((2, sums.shape[1]), jnp.float32),
        ),
        in_specs=[here, here],
        out_specs=(here, here),
        compiler_params=pltpu.CompilerParams(vmem_limit_bytes=VMEM_LIMIT // 4),
        name="final_sums",
    )(weight, sums)


def all_steps(
    pair_window, tri_cotangent, saved_left, saved_right, norm_gain, norm_bias, proj_weight
):
    block_count, own_rows, col_tokens, channels = tri_cotangent.shape
    window_len = saved_left.shape[2]
    cols = lax.axis_size("col")
    rows = lax.axis_size("row")
    lines_y = [[x * (rows // 2) + y for y in range(rows // 2)] for x in range(2)]
    lines_z = [[z * 4 + k for z in range(cols // 4)] for k in range(4)]
    one_core = [[c for c in range(cols) if c % 2 == k] for k in range(2)]
    right_near = jnp.broadcast_to(saved_right, (rows // 2, *saved_right.shape[1:]))
    right_near = lax.all_to_all(
        right_near, "row", 0, 0, tiled=True, axis_index_groups=lines_y
    )
    right_far = exchanged(right_near, "row", rows // 2)
    cot_turned = lax.optimization_barrier(
        jnp.transpose(
            tri_cotangent.reshape(block_count * own_rows, col_tokens, channels), (2, 1, 0)
        )
    )
    own = jnp.broadcast_to(saved_left, (cols // 4, *saved_left.shape[1:]))
    own = lax.all_to_all(own, "col", 0, 0, tiled=True, axis_index_groups=lines_z)
    own = own.reshape(cols // 4, own_rows * window_len, channels)
    flat = (-1, channels)
    kept, away = left_parts(
        right_near.reshape(flat), right_far.reshape(flat), cot_turned, cols, window_len
    )
    came = exchanged(away, "col", 1)
    chip_part = pair_sum(kept, came)
    left_arrived = lax.all_to_all(chip_part, "col", 0, 0, tiled=True, axis_index_groups=one_core)
    across = exchanged(own, "col", 2)
    own_pair = exchanged(own, "col", 1)
    across_pair = exchanged(across, "col", 1)
    right_part = right_parts((own, across, own_pair, across_pair), cot_turned, window_len)
    right_part = right_part.reshape(col_tokens, window_len, channels)
    left_grad = left_arrived.astype(jnp.float32).sum(axis=0)
    right_grad = sent_and_summed(right_part, "row", 0)
    positions = own_rows * window_len
    pair_grad, weight_part, norm_part = gated_norm_back(
        pair_window.reshape(positions, pair_window.shape[3]),
        left_grad.reshape(positions, channels),
        right_grad.reshape(positions, channels),
        norm_gain,
        norm_bias,
        proj_weight,
    )
    pair_grad, weight_part, norm_part = lax.optimization_barrier(
        (pair_grad, weight_part, norm_part)
    )
    weight_grad, norm_grad = summed_over_all(weight_part, norm_part)
    return (pair_grad.reshape(pair_window.shape), weight_grad, norm_grad)


def solution(mesh):
    return jax.shard_map(
        all_steps,
        mesh=mesh,
        in_specs=(
            P("col", "row", None, None),
            P(None, "row", "col", None),
            P("col", "row", None, None),
            P("col", "row", None, None),
            P(),
            P(),
            P(),
        ),
        out_specs=(P("col", "row", None, None), P(), P()),
        check_vma=False,
    )
```

```python
import functools

import jax
import jax.numpy as jnp
from jax import lax
from jax.experimental import pallas as pl
from jax.experimental.pallas import tpu as pltpu
from jax.sharding import PartitionSpec as P


def sent_to_all(x, axis):
    devices = lax.axis_size(axis)
    return lax.all_to_all(jnp.broadcast_to(x[None], (devices, *x.shape)), axis, 0, 0, tiled=True)


def split_up(x, dim, devices):
    lengths = x.shape
    parts = x.reshape(*lengths[:dim], devices, lengths[dim] // devices, *lengths[dim + 1 :])
    return jnp.moveaxis(parts, dim, 0)


def sent_and_summed(x, axis, dim):
    parts = split_up(x, dim, lax.axis_size(axis))
    arrived = lax.all_to_all(parts, axis, split_axis=0, concat_axis=0, tiled=True)
    return arrived.astype(jnp.float32).sum(axis=0)


def gated_norm_back(pair_rows, left_grad, right_grad, norm_gain, norm_bias, proj_weight):
    pair = pair_rows.astype(jnp.float32)
    average = jnp.mean(pair, axis=-1, keepdims=True)
    centred = pair - average
    variance = jnp.mean(centred * centred, axis=-1, keepdims=True)
    inv_std = lax.rsqrt(variance + 1e-05)
    unit_pair = centred * inv_std
    normed = (unit_pair * norm_gain + norm_bias).astype(jnp.bfloat16)
    chans = proj_weight.shape[2]
    stacked = jnp.transpose(proj_weight, (1, 0, 2)).reshape(proj_weight.shape[1], 4 * chans)
    preact = jnp.dot(normed, stacked, preferred_element_type=jnp.float32)
    gate_left = jax.nn.sigmoid(preact[:, :chans])
    value_left = preact[:, chans : 2 * chans]
    gate_right = jax.nn.sigmoid(preact[:, 2 * chans : 3 * chans])
    value_right = preact[:, 3 * chans :]
    pre_grads = jnp.concatenate(
        [
            left_grad * value_left * gate_left * (1.0 - gate_left),
            left_grad * gate_left,
            right_grad * value_right * gate_right * (1.0 - gate_right),
            right_grad * gate_right,
        ],
        axis=1,
    ).astype(jnp.bfloat16)
    weight_part = lax.dot_general(
        normed, pre_grads, (((0,), (0,)), ((), ())), preferred_element_type=jnp.float32
    )
    weight_part = jnp.transpose(weight_part.reshape(proj_weight.shape[1], 4, chans), (1, 0, 2))
    normed_grad = jnp.dot(pre_grads, stacked.T, preferred_element_type=jnp.float32)
    norm_part = jnp.stack([jnp.sum(normed_grad * unit_pair, axis=0), jnp.sum(normed_grad, axis=0)])
    scaled_grad = normed_grad * norm_gain
    pair_grad = inv_std * (
        scaled_grad
        - jnp.mean(scaled_grad, axis=-1, keepdims=True)
        - unit_pair * jnp.mean(scaled_grad * unit_pair, axis=-1, keepdims=True)
    )
    return (pair_grad, weight_part, norm_part)


def with_split_norm(part, rows):
    norm = part[rows : rows + 2] + part[rows + 2 : rows + 4]
    return jnp.concatenate([part[:rows], split_in_two(norm)], axis=0).astype(jnp.bfloat16)


def split_in_two(norm):
    high = lax.reduce_precision(norm, 8, 7)
    return jnp.concatenate([high, norm - high, jnp.zeros((4, norm.shape[1]), norm.dtype)], axis=0)


def summed_over_all(weight_part, norm_part, pair_grad):
    cols = lax.axis_size("col")
    shape = weight_part.shape
    width = shape[-1]
    chunks = weight_part.reshape(cols, -1, width).astype(jnp.bfloat16)
    rows = chunks.shape[1]
    extra = split_in_two(norm_part).astype(jnp.bfloat16)
    packed = jnp.concatenate([chunks, jnp.broadcast_to(extra[None], (cols, 8, width))], axis=1)
    arrived = lax.all_to_all(packed, "col", 0, 0, tiled=True)
    part = arrived.astype(jnp.float32).sum(axis=0)
    whole = sent_to_all(with_split_norm(part, rows), "row").astype(jnp.float32).sum(axis=0)
    chunk, sums = lax.optimization_barrier((whole[:rows].astype(jnp.bfloat16), whole[rows:]))
    weight_grad = sent_to_all(chunk, "col").reshape(-1, width)
    weight_grad, norm_grad, pair_grad = final_sums(weight_grad, sums, pair_grad)
    return weight_grad.reshape(shape), norm_grad, pair_grad


def exchanged(x, axis, step):
    devices = lax.axis_size(axis)
    return lax.ppermute(x, axis, [(d, d ^ step) for d in range(devices)])


PAD = 8
VMEM_LIMIT = 24 * 2**20
ROWS_TURNED = (((1,), (1,)), ((), ()))


def turned(x):
    n = x.shape[1]
    eye = lax.broadcasted_iota(jnp.int32, (n, n), 0) == lax.broadcasted_iota(jnp.int32, (n, n), 1)
    return lax.dot_general(
        eye.astype(jnp.float32).astype(jnp.bfloat16),
        x,
        ROWS_TURNED,
        preferred_element_type=jnp.float32,
    )


def place_of():
    row, col = lax.axis_index("row"), lax.axis_index("col")
    half = lax.axis_size("row") // 2
    return lax.div(row, half), lax.rem(lax.div(col, 2), 2), lax.rem(col, 2)


def left_kernel(window_len, near_ref, far_ref, cot_ref, kept_ref, away_ref, *scratch):
    wide, by_key, product, rows_out = scratch
    hidden, cols, rows = cot_ref.shape
    x_high, _, core = place_of()
    group, step = window_len + PAD, hidden + PAD
    for source, half in ((near_ref, x_high), (far_ref, 1 - x_high)):
        for j in range(cols // 2):
            at = pl.multiple_of((half * (cols // 2) + j) * group, 8)
            wide[pl.ds(at, window_len), :] = source[pl.ds(j * window_len, window_len), :].astype(
                jnp.float32
            )
    for k in range(window_len):
        by_key[pl.ds(k * step, hidden), :] = turned(
            wide[pl.ds(k, cols, stride=group), :].astype(jnp.bfloat16)
        )
    for h in range(hidden):
        keys = by_key[pl.ds(h, window_len, stride=step), :].astype(jnp.bfloat16)
        product[pl.ds(h, window_len, stride=step), :] = jnp.dot(
            keys, cot_ref[h], preferred_element_type=jnp.float32
        )
    for k in range(window_len):
        rows_out[pl.ds(k, rows, stride=group), :] = turned(
            product[pl.ds(k * step, hidden), :].astype(jnp.bfloat16)
        )
    tokens = kept_ref.shape[1] // window_len
    for target, side in ((kept_ref, core), (away_ref, 1 - core)):
        for q in range(kept_ref.shape[0]):
            for t in range(tokens):
                at = pl.multiple_of(((2 * q + side) * tokens + t) * group, 8)
                target[q, pl.ds(t * window_len, window_len), :] = rows_out[
                    pl.ds(at, window_len), :
                ].astype(jnp.bfloat16)


def left_parts(near, far, cot_turned, blocks, window_len):
    hidden, cols, rows = cot_turned.shape
    group, step = window_len + PAD, hidden + PAD
    out = jax.ShapeDtypeStruct((blocks // 2, rows * window_len // blocks, hidden), jnp.bfloat16)
    here = pl.BlockSpec(memory_space=pltpu.VMEM)
    return pl.pallas_call(
        functools.partial(left_kernel, window_len),
        out_shape=(out, out),
        in_specs=[here, here, here],
        out_specs=(here, here),
        scratch_shapes=[
            pltpu.VMEM((cols * group, hidden), jnp.float32),
            pltpu.VMEM((window_len * step, cols), jnp.float32),
            pltpu.VMEM((window_len * step, rows), jnp.float32),
            pltpu.VMEM((rows * group, hidden), jnp.float32),
        ],
        compiler_params=pltpu.CompilerParams(vmem_limit_bytes=VMEM_LIMIT),
        name="left_parts",
    )(near, far, cot_turned)


def right_kernel(window_len, own_ref, x_ref, core_ref, both_ref, cot_ref, out_ref, *scratch):
    wide, by_key, product, rows_out = scratch
    hidden, cols, rows = cot_ref.shape
    _, x_low, core = place_of()
    group, step = window_len + PAD, hidden + PAD
    tokens = own_ref.shape[1] // window_len
    for source, x, side in (
        (own_ref, x_low, core),
        (x_ref, 1 - x_low, core),
        (core_ref, x_low, 1 - core),
        (both_ref, 1 - x_low, 1 - core),
    ):
        for z in range(own_ref.shape[0]):
            for t in range(tokens):
                at = pl.multiple_of(((z * 4 + 2 * x + side) * tokens + t) * group, 8)
                wide[pl.ds(at, window_len), :] = source[
                    z, pl.ds(t * window_len, window_len), :
                ].astype(jnp.float32)
    for k in range(window_len):
        by_key[pl.ds(k * step, hidden), :] = turned(
            wide[pl.ds(k, rows, stride=group), :].astype(jnp.bfloat16)
        )
    for h in range(hidden):
        keys = by_key[pl.ds(h, window_len, stride=step), :].astype(jnp.bfloat16)
        product[pl.ds(h, window_len, stride=step), :] = lax.dot_general(
            keys, cot_ref[h], ROWS_TURNED, preferred_element_type=jnp.float32
        )
    for k in range(window_len):
        rows_out[pl.ds(k, cols, stride=group), :] = turned(
            product[pl.ds(k * step, hidden), :].astype(jnp.bfloat16)
        )
    for j in range(cols):
        out_ref[pl.ds(j * window_len, window_len), :] = rows_out[
            pl.ds(j * group, window_len), :
        ].astype(jnp.bfloat16)


def right_parts(pieces, cot_turned, window_len):
    hidden, cols, rows = cot_turned.shape
    group, step = window_len + PAD, hidden + PAD
    here = pl.BlockSpec(memory_space=pltpu.VMEM)
    return pl.pallas_call(
        functools.partial(right_kernel, window_len),
        out_shape=jax.ShapeDtypeStruct((cols * window_len, hidden), jnp.bfloat16),
        in_specs=[here, here, here, here, here],
        out_specs=here,
        scratch_shapes=[
            pltpu.VMEM((rows * group, hidden), jnp.float32),
            pltpu.VMEM((window_len * step, rows), jnp.float32),
            pltpu.VMEM((window_len * step, cols), jnp.float32),
            pltpu.VMEM((cols * group, hidden), jnp.float32),
        ],
        compiler_params=pltpu.CompilerParams(vmem_limit_bytes=VMEM_LIMIT),
        name="right_parts",
    )(*pieces, cot_turned)


def spread_kernel(x_ref, out_ref, done):
    copies = [
        pltpu.make_async_copy(x_ref, out_ref.at[n], done.at[n]) for n in range(out_ref.shape[0])
    ]
    for copy in copies:
        copy.start()
    for copy in copies:
        copy.wait()


def spread(x, count):
    anywhere = pl.BlockSpec(memory_space=pl.ANY)
    return pl.pallas_call(
        spread_kernel,
        out_shape=jax.ShapeDtypeStruct((count, *x.shape), x.dtype),
        in_specs=[anywhere],
        out_specs=anywhere,
        scratch_shapes=[pltpu.SemaphoreType.DMA((count,))],
        compiler_params=pltpu.CompilerParams(vmem_limit_bytes=VMEM_LIMIT // 4),
        name="spread",
    )(x)


def pair_kernel(kept_ref, came_ref, out_ref):
    total = kept_ref[...].astype(jnp.float32) + came_ref[...].astype(jnp.float32)
    out_ref[...] = total.astype(jnp.bfloat16)


def pair_sum(kept, came):
    block = pl.BlockSpec((kept.shape[0] // 4, *kept.shape[1:]), lambda i: (i, 0, 0))
    return pl.pallas_call(
        pair_kernel,
        grid=(4,),
        out_shape=jax.ShapeDtypeStruct(kept.shape, kept.dtype),
        in_specs=[block, block],
        out_specs=block,
        compiler_params=pltpu.CompilerParams(vmem_limit_bytes=VMEM_LIMIT // 4),
        name="pair_sum",
    )(kept, came)


def final_kernel(weight_ref, sums_ref, pair_ref, weight_out, norm_out, pair_out):
    pair_out[...] = pair_ref[...].astype(jnp.bfloat16)
    weight_out[...] = weight_ref[...].astype(jnp.float32)
    norm_out[...] = sums_ref[0:2, :] + sums_ref[2:4, :]


def final_sums(weight, sums, pair):
    here = pl.BlockSpec(memory_space=pltpu.VMEM)
    return pl.pallas_call(
        final_kernel,
        out_shape=(
            jax.ShapeDtypeStruct(weight.shape, jnp.float32),
            jax.ShapeDtypeStruct((2, sums.shape[1]), jnp.float32),
            jax.ShapeDtypeStruct(pair.shape, jnp.bfloat16),
        ),
        in_specs=[here, here, here],
        out_specs=(here, here, here),
        compiler_params=pltpu.CompilerParams(vmem_limit_bytes=VMEM_LIMIT // 4),
        name="final_sums",
    )(weight, sums, pair)


def all_steps(
    pair_window, tri_cotangent, saved_left, saved_right, norm_gain, norm_bias, proj_weight
):
    block_count, own_rows, col_tokens, channels = tri_cotangent.shape
    window_len = saved_left.shape[2]
    cols = lax.axis_size("col")
    rows = lax.axis_size("row")
    lines_y = [[x * (rows // 2) + y for y in range(rows // 2)] for x in range(2)]
    lines_z = [[z * 4 + k for z in range(cols // 4)] for k in range(4)]
    one_core = [[c for c in range(cols) if c % 2 == k] for k in range(2)]
    right_near = spread(saved_right[0], rows // 2)
    right_near = lax.all_to_all(
        right_near, "row", 0, 0, tiled=True, axis_index_groups=lines_y
    )
    right_far = exchanged(right_near, "row", rows // 2)
    cot_turned = lax.optimization_barrier(
        jnp.transpose(
            tri_cotangent.reshape(block_count * own_rows, col_tokens, channels), (2, 1, 0)
        )
    )
    own = jnp.broadcast_to(saved_left, (cols // 4, *saved_left.shape[1:]))
    own = lax.all_to_all(own, "col", 0, 0, tiled=True, axis_index_groups=lines_z)
    own = own.reshape(cols // 4, own_rows * window_len, channels)
    flat = (-1, channels)
    kept, away = left_parts(
        right_near.reshape(flat), right_far.reshape(flat), cot_turned, cols, window_len
    )
    came = exchanged(away, "col", 1)
    chip_part = pair_sum(kept, came)
    left_arrived = lax.all_to_all(chip_part, "col", 0, 0, tiled=True, axis_index_groups=one_core)
    across = exchanged(own, "col", 2)
    own_pair = exchanged(own, "col", 1)
    across_pair = exchanged(across, "col", 1)
    right_part = right_parts((own, across, own_pair, across_pair), cot_turned, window_len)
    right_part = right_part.reshape(col_tokens, window_len, channels)
    left_grad = left_arrived.astype(jnp.float32).sum(axis=0)
    right_grad = sent_and_summed(right_part, "row", 0)
    positions = own_rows * window_len
    pair_grad, weight_part, norm_part = gated_norm_back(
        pair_window.reshape(positions, pair_window.shape[3]),
        left_grad.reshape(positions, channels),
        right_grad.reshape(positions, channels),
        norm_gain,
        norm_bias,
        proj_weight,
    )
    pair_grad, weight_part, norm_part = lax.optimization_barrier(
        (pair_grad, weight_part, norm_part)
    )
    weight_grad, norm_grad, pair_grad = summed_over_all(weight_part, norm_part, pair_grad)
    return (pair_grad.reshape(pair_window.shape), weight_grad, norm_grad)


def solution(mesh):
    return jax.shard_map(
        all_steps,
        mesh=mesh,
        in_specs=(
            P("col", "row", None, None),
            P(None, "row", "col", None),
            P("col", "row", None, None),
            P("col", "row", None, None),
            P(),
            P(),
            P(),
        ),
        out_specs=(P("col", "row", None, None), P(), P()),
        check_vma=False,
    )
```

```python
import functools

import jax
import jax.numpy as jnp
from jax import lax
from jax.experimental import pallas as pl
from jax.experimental.pallas import tpu as pltpu
from jax.sharding import PartitionSpec as P


def sent_to_all(x, axis):
    devices = lax.axis_size(axis)
    return lax.all_to_all(jnp.broadcast_to(x[None], (devices, *x.shape)), axis, 0, 0, tiled=True)


def split_up(x, dim, devices):
    lengths = x.shape
    parts = x.reshape(*lengths[:dim], devices, lengths[dim] // devices, *lengths[dim + 1 :])
    return jnp.moveaxis(parts, dim, 0)


def sent_and_summed(x, axis, dim):
    parts = split_up(x, dim, lax.axis_size(axis))
    arrived = lax.all_to_all(parts, axis, split_axis=0, concat_axis=0, tiled=True)
    return arrived.astype(jnp.float32).sum(axis=0)


def gated_norm_back(pair_rows, left_grad, right_grad, norm_gain, norm_bias, proj_weight):
    pair = pair_rows.astype(jnp.float32)
    average = jnp.mean(pair, axis=-1, keepdims=True)
    centred = pair - average
    variance = jnp.mean(centred * centred, axis=-1, keepdims=True)
    inv_std = lax.rsqrt(variance + 1e-05)
    unit_pair = centred * inv_std
    normed = (unit_pair * norm_gain + norm_bias).astype(jnp.bfloat16)
    chans = proj_weight.shape[2]
    stacked = jnp.transpose(proj_weight, (1, 0, 2)).reshape(proj_weight.shape[1], 4 * chans)
    preact = jnp.dot(normed, stacked, preferred_element_type=jnp.float32)
    gate_left = jax.nn.sigmoid(preact[:, :chans])
    value_left = preact[:, chans : 2 * chans]
    gate_right = jax.nn.sigmoid(preact[:, 2 * chans : 3 * chans])
    value_right = preact[:, 3 * chans :]
    pre_grads = jnp.concatenate(
        [
            left_grad * value_left * gate_left * (1.0 - gate_left),
            left_grad * gate_left,
            right_grad * value_right * gate_right * (1.0 - gate_right),
            right_grad * gate_right,
        ],
        axis=1,
    ).astype(jnp.bfloat16)
    weight_part = lax.dot_general(
        normed, pre_grads, (((0,), (0,)), ((), ())), preferred_element_type=jnp.float32
    )
    weight_part = jnp.transpose(weight_part.reshape(proj_weight.shape[1], 4, chans), (1, 0, 2))
    normed_grad = jnp.dot(pre_grads, stacked.T, preferred_element_type=jnp.float32)
    norm_part = jnp.stack([jnp.sum(normed_grad * unit_pair, axis=0), jnp.sum(normed_grad, axis=0)])
    scaled_grad = normed_grad * norm_gain
    pair_grad = inv_std * (
        scaled_grad
        - jnp.mean(scaled_grad, axis=-1, keepdims=True)
        - unit_pair * jnp.mean(scaled_grad * unit_pair, axis=-1, keepdims=True)
    )
    return (pair_grad, weight_part, norm_part)


def with_split_norm(part, rows):
    norm = part[rows : rows + 2] + part[rows + 2 : rows + 4]
    return jnp.concatenate([part[:rows], split_in_two(norm)], axis=0).astype(jnp.bfloat16)


def split_in_two(norm):
    high = lax.reduce_precision(norm, 8, 7)
    return jnp.concatenate([high, norm - high, jnp.zeros((4, norm.shape[1]), norm.dtype)], axis=0)


def summed_over_all(weight_part, norm_part, pair_grad):
    cols = lax.axis_size("col")
    shape = weight_part.shape
    width = shape[-1]
    chunks = weight_part.reshape(cols, -1, width).astype(jnp.bfloat16)
    rows = chunks.shape[1]
    extra = split_in_two(norm_part).astype(jnp.bfloat16)
    packed = jnp.concatenate([chunks, jnp.broadcast_to(extra[None], (cols, 8, width))], axis=1)
    arrived = lax.all_to_all(packed, "col", 0, 0, tiled=True)
    part = arrived.astype(jnp.float32).sum(axis=0)
    whole = sent_to_all(with_split_norm(part, rows), "row").astype(jnp.float32).sum(axis=0)
    chunk, sums = lax.optimization_barrier((whole[:rows].astype(jnp.bfloat16), whole[rows:]))
    weight_grad = sent_to_all(chunk, "col").reshape(-1, width)
    weight_grad, norm_grad, pair_grad = final_sums(weight_grad, sums, pair_grad)
    return weight_grad.reshape(shape), norm_grad, pair_grad


def exchanged(x, axis, step):
    devices = lax.axis_size(axis)
    return lax.ppermute(x, axis, [(d, d ^ step) for d in range(devices)])


PAD = 8
VMEM_LIMIT = 24 * 2**20
ROWS_TURNED = (((1,), (1,)), ((), ()))


def turned(x):
    n = x.shape[1]
    eye = lax.broadcasted_iota(jnp.int32, (n, n), 0) == lax.broadcasted_iota(jnp.int32, (n, n), 1)
    return lax.dot_general(
        eye.astype(jnp.float32).astype(jnp.bfloat16),
        x,
        ROWS_TURNED,
        preferred_element_type=jnp.float32,
    )


def place_of():
    row, col = lax.axis_index("row"), lax.axis_index("col")
    half = lax.axis_size("row") // 2
    return lax.div(row, half), lax.rem(lax.div(col, 2), 2), lax.rem(col, 2)


def left_kernel(window_len, near_ref, far_ref, cot_ref, kept_ref, away_ref, *scratch):
    wide, by_key, product, rows_out = scratch
    hidden, cols, rows = cot_ref.shape
    x_high, _, core = place_of()
    group, step = window_len + PAD, hidden + PAD
    for source, half in ((near_ref, x_high), (far_ref, 1 - x_high)):
        for j in range(cols // 2):
            at = pl.multiple_of((half * (cols // 2) + j) * group, 8)
            wide[pl.ds(at, window_len), :] = source[pl.ds(j * window_len, window_len), :].astype(
                jnp.float32
            )
    for k in range(window_len):
        by_key[pl.ds(k * step, hidden), :] = turned(
            wide[pl.ds(k, cols, stride=group), :].astype(jnp.bfloat16)
        )
    for h in range(hidden):
        keys = by_key[pl.ds(h, window_len, stride=step), :].astype(jnp.bfloat16)
        product[pl.ds(h, window_len, stride=step), :] = jnp.dot(
            keys, cot_ref[h], preferred_element_type=jnp.float32
        )
    for k in range(window_len):
        rows_out[pl.ds(k, rows, stride=group), :] = turned(
            product[pl.ds(k * step, hidden), :].astype(jnp.bfloat16)
        )
    tokens = kept_ref.shape[1] // window_len
    for target, side in ((kept_ref, core), (away_ref, 1 - core)):
        for q in range(kept_ref.shape[0]):
            for t in range(tokens):
                at = pl.multiple_of(((2 * q + side) * tokens + t) * group, 8)
                target[q, pl.ds(t * window_len, window_len), :] = rows_out[
                    pl.ds(at, window_len), :
                ].astype(jnp.bfloat16)


def left_parts(near, far, cot_turned, blocks, window_len):
    hidden, cols, rows = cot_turned.shape
    group, step = window_len + PAD, hidden + PAD
    out = jax.ShapeDtypeStruct((blocks // 2, rows * window_len // blocks, hidden), jnp.bfloat16)
    here = pl.BlockSpec(memory_space=pltpu.VMEM)
    return pl.pallas_call(
        functools.partial(left_kernel, window_len),
        out_shape=(out, out),
        in_specs=[here, here, here],
        out_specs=(here, here),
        scratch_shapes=[
            pltpu.VMEM((cols * group, hidden), jnp.float32),
            pltpu.VMEM((window_len * step, cols), jnp.float32),
            pltpu.VMEM((window_len * step, rows), jnp.float32),
            pltpu.VMEM((rows * group, hidden), jnp.float32),
        ],
        compiler_params=pltpu.CompilerParams(vmem_limit_bytes=VMEM_LIMIT),
        name="left_parts",
    )(near, far, cot_turned)


def right_kernel(window_len, own_ref, x_ref, core_ref, both_ref, cot_ref, out_ref, *scratch):
    wide, by_key, product, rows_out = scratch
    hidden, cols, rows = cot_ref.shape
    _, x_low, core = place_of()
    group, step = window_len + PAD, hidden + PAD
    tokens = own_ref.shape[1] // window_len
    for source, x, side in (
        (own_ref, x_low, core),
        (x_ref, 1 - x_low, core),
        (core_ref, x_low, 1 - core),
        (both_ref, 1 - x_low, 1 - core),
    ):
        for z in range(own_ref.shape[0]):
            for t in range(tokens):
                at = pl.multiple_of(((z * 4 + 2 * x + side) * tokens + t) * group, 8)
                wide[pl.ds(at, window_len), :] = source[
                    z, pl.ds(t * window_len, window_len), :
                ].astype(jnp.float32)
    for k in range(window_len):
        by_key[pl.ds(k * step, hidden), :] = turned(
            wide[pl.ds(k, rows, stride=group), :].astype(jnp.bfloat16)
        )
    for h in range(hidden):
        keys = by_key[pl.ds(h, window_len, stride=step), :].astype(jnp.bfloat16)
        product[pl.ds(h, window_len, stride=step), :] = lax.dot_general(
            keys, cot_ref[h], ROWS_TURNED, preferred_element_type=jnp.float32
        )
    for k in range(window_len):
        rows_out[pl.ds(k, cols, stride=group), :] = turned(
            product[pl.ds(k * step, hidden), :].astype(jnp.bfloat16)
        )
    for j in range(cols):
        out_ref[pl.ds(j * window_len, window_len), :] = rows_out[
            pl.ds(j * group, window_len), :
        ].astype(jnp.bfloat16)


def right_parts(pieces, cot_turned, window_len):
    hidden, cols, rows = cot_turned.shape
    group, step = window_len + PAD, hidden + PAD
    here = pl.BlockSpec(memory_space=pltpu.VMEM)
    return pl.pallas_call(
        functools.partial(right_kernel, window_len),
        out_shape=jax.ShapeDtypeStruct((cols * window_len, hidden), jnp.bfloat16),
        in_specs=[here, here, here, here, here],
        out_specs=here,
        scratch_shapes=[
            pltpu.VMEM((rows * group, hidden), jnp.float32),
            pltpu.VMEM((window_len * step, rows), jnp.float32),
            pltpu.VMEM((window_len * step, cols), jnp.float32),
            pltpu.VMEM((cols * group, hidden), jnp.float32),
        ],
        compiler_params=pltpu.CompilerParams(vmem_limit_bytes=VMEM_LIMIT),
        name="right_parts",
    )(*pieces, cot_turned)


def pair_kernel(kept_ref, came_hbm, out_hbm, came, out, arrived, left):
    blocks = arrived.shape[0]
    size = kept_ref.shape[0] // blocks
    parts = [pl.ds(n * size, size) for n in range(blocks)]
    incoming = [
        pltpu.make_async_copy(came_hbm.at[part], came.at[part], arrived.at[n])
        for n, part in enumerate(parts)
    ]
    outgoing = [
        pltpu.make_async_copy(out.at[part], out_hbm.at[part], left.at[n])
        for n, part in enumerate(parts)
    ]
    for copy in incoming:
        copy.start()
    for n, part in enumerate(parts):
        incoming[n].wait()
        total = kept_ref[part].astype(jnp.float32) + came[part].astype(jnp.float32)
        out[part] = total.astype(jnp.bfloat16)
        outgoing[n].start()
    for copy in outgoing:
        copy.wait()


def pair_sum(kept, came):
    here, anywhere = pl.BlockSpec(memory_space=pltpu.VMEM), pl.BlockSpec(memory_space=pl.ANY)
    return pl.pallas_call(
        pair_kernel,
        out_shape=jax.ShapeDtypeStruct(kept.shape, kept.dtype),
        in_specs=[here, anywhere],
        out_specs=anywhere,
        scratch_shapes=[
            pltpu.VMEM(kept.shape, kept.dtype),
            pltpu.VMEM(kept.shape, kept.dtype),
            pltpu.SemaphoreType.DMA((4,)),
            pltpu.SemaphoreType.DMA((4,)),
        ],
        compiler_params=pltpu.CompilerParams(vmem_limit_bytes=VMEM_LIMIT // 4),
        name="pair_sum",
    )(kept, came)


def final_kernel(weight_ref, sums_ref, pair_ref, weight_out, norm_out, pair_out):
    pair_out[...] = pair_ref[...].astype(jnp.bfloat16)
    weight_out[...] = weight_ref[...].astype(jnp.float32)
    norm_out[...] = sums_ref[0:2, :] + sums_ref[2:4, :]


def final_sums(weight, sums, pair):
    here = pl.BlockSpec(memory_space=pltpu.VMEM)
    return pl.pallas_call(
        final_kernel,
        out_shape=(
            jax.ShapeDtypeStruct(weight.shape, jnp.float32),
            jax.ShapeDtypeStruct((2, sums.shape[1]), jnp.float32),
            jax.ShapeDtypeStruct(pair.shape, jnp.bfloat16),
        ),
        in_specs=[here, here, here],
        out_specs=(here, here, here),
        compiler_params=pltpu.CompilerParams(vmem_limit_bytes=VMEM_LIMIT // 4),
        name="final_sums",
    )(weight, sums, pair)


def all_steps(
    pair_window, tri_cotangent, saved_left, saved_right, norm_gain, norm_bias, proj_weight
):
    block_count, own_rows, col_tokens, channels = tri_cotangent.shape
    window_len = saved_left.shape[2]
    cols = lax.axis_size("col")
    rows = lax.axis_size("row")
    lines_y = [[x * (rows // 2) + y for y in range(rows // 2)] for x in range(2)]
    lines_z = [[z * 4 + k for z in range(cols // 4)] for k in range(4)]
    one_core = [[c for c in range(cols) if c % 2 == k] for k in range(2)]
    right_near = jnp.broadcast_to(saved_right, (rows // 2, *saved_right.shape[1:]))
    right_near = lax.all_to_all(
        right_near, "row", 0, 0, tiled=True, axis_index_groups=lines_y
    )
    right_far = exchanged(right_near, "row", rows // 2)
    cot_turned = lax.optimization_barrier(
        jnp.transpose(
            tri_cotangent.reshape(block_count * own_rows, col_tokens, channels), (2, 1, 0)
        )
    )
    own = jnp.broadcast_to(saved_left, (cols // 4, *saved_left.shape[1:]))
    own = lax.all_to_all(own, "col", 0, 0, tiled=True, axis_index_groups=lines_z)
    own = own.reshape(cols // 4, own_rows * window_len, channels)
    flat = (-1, channels)
    kept, away = left_parts(
        right_near.reshape(flat), right_far.reshape(flat), cot_turned, cols, window_len
    )
    came = exchanged(away, "col", 1)
    chip_part = pair_sum(kept, came)
    left_arrived = lax.all_to_all(chip_part, "col", 0, 0, tiled=True, axis_index_groups=one_core)
    across = exchanged(own, "col", 2)
    own_pair = exchanged(own, "col", 1)
    across_pair = exchanged(across, "col", 1)
    right_part = right_parts((own, across, own_pair, across_pair), cot_turned, window_len)
    right_part = right_part.reshape(col_tokens, window_len, channels)
    left_grad = left_arrived.astype(jnp.float32).sum(axis=0)
    right_grad = sent_and_summed(right_part, "row", 0)
    positions = own_rows * window_len
    pair_grad, weight_part, norm_part = gated_norm_back(
        pair_window.reshape(positions, pair_window.shape[3]),
        left_grad.reshape(positions, channels),
        right_grad.reshape(positions, channels),
        norm_gain,
        norm_bias,
        proj_weight,
    )
    pair_grad, weight_part, norm_part = lax.optimization_barrier(
        (pair_grad, weight_part, norm_part)
    )
    weight_grad, norm_grad, pair_grad = summed_over_all(weight_part, norm_part, pair_grad)
    return (pair_grad.reshape(pair_window.shape), weight_grad, norm_grad)


def solution(mesh):
    return jax.shard_map(
        all_steps,
        mesh=mesh,
        in_specs=(
            P("col", "row", None, None),
            P(None, "row", "col", None),
            P("col", "row", None, None),
            P("col", "row", None, None),
            P(),
            P(),
            P(),
        ),
        out_specs=(P("col", "row", None, None), P(), P()),
        check_vma=False,
    )
```

```python
import functools

import jax
import jax.numpy as jnp
from jax import lax
from jax.experimental import pallas as pl
from jax.experimental.pallas import tpu as pltpu
from jax.sharding import PartitionSpec as P


def split_up(x, dim, devices):
    lengths = x.shape
    parts = x.reshape(*lengths[:dim], devices, lengths[dim] // devices, *lengths[dim + 1 :])
    return jnp.moveaxis(parts, dim, 0)


def sent_and_summed(x, axis, dim):
    parts = split_up(x, dim, lax.axis_size(axis))
    arrived = lax.all_to_all(parts, axis, split_axis=0, concat_axis=0, tiled=True)
    return arrived.astype(jnp.float32).sum(axis=0)


def gated_norm_back(pair_rows, left_grad, right_grad, norm_gain, norm_bias, proj_weight):
    pair = pair_rows.astype(jnp.float32)
    average = jnp.mean(pair, axis=-1, keepdims=True)
    centred = pair - average
    variance = jnp.mean(centred * centred, axis=-1, keepdims=True)
    inv_std = lax.rsqrt(variance + 1e-05)
    unit_pair = centred * inv_std
    normed = (unit_pair * norm_gain + norm_bias).astype(jnp.bfloat16)
    chans = proj_weight.shape[2]
    stacked = jnp.transpose(proj_weight, (1, 0, 2)).reshape(proj_weight.shape[1], 4 * chans)
    preact = jnp.dot(normed, stacked, preferred_element_type=jnp.float32)
    gate_left = jax.nn.sigmoid(preact[:, :chans])
    value_left = preact[:, chans : 2 * chans]
    gate_right = jax.nn.sigmoid(preact[:, 2 * chans : 3 * chans])
    value_right = preact[:, 3 * chans :]
    pre_grads = jnp.concatenate(
        [
            left_grad * value_left * gate_left * (1.0 - gate_left),
            left_grad * gate_left,
            right_grad * value_right * gate_right * (1.0 - gate_right),
            right_grad * gate_right,
        ],
        axis=1,
    ).astype(jnp.bfloat16)
    weight_part = lax.dot_general(
        normed, pre_grads, (((0,), (0,)), ((), ())), preferred_element_type=jnp.float32
    )
    weight_part = jnp.transpose(weight_part.reshape(proj_weight.shape[1], 4, chans), (1, 0, 2))
    normed_grad = jnp.dot(pre_grads, stacked.T, preferred_element_type=jnp.float32)
    norm_part = jnp.stack([jnp.sum(normed_grad * unit_pair, axis=0), jnp.sum(normed_grad, axis=0)])
    scaled_grad = normed_grad * norm_gain
    pair_grad = inv_std * (
        scaled_grad
        - jnp.mean(scaled_grad, axis=-1, keepdims=True)
        - unit_pair * jnp.mean(scaled_grad * unit_pair, axis=-1, keepdims=True)
    )
    return (pair_grad, weight_part, norm_part)


def with_split_norm(part, rows):
    norm = part[rows : rows + 2] + part[rows + 2 : rows + 4]
    return jnp.concatenate([part[:rows], split_in_two(norm)], axis=0).astype(jnp.bfloat16)


def split_in_two(norm):
    high = lax.reduce_precision(norm, 8, 7)
    return jnp.concatenate([high, norm - high, jnp.zeros((4, norm.shape[1]), norm.dtype)], axis=0)


def summed_over_all(weight_part, norm_part, pair_grad):
    half, cols = lax.axis_size("row") // 2, lax.axis_size("col")
    members = 2 * cols
    lines_y = [[x * half + y for y in range(half)] for x in range(2)]
    planes = [
        [(x * half + y) * cols + c for x in range(2) for c in range(cols)] for y in range(half)
    ]
    shape = weight_part.shape
    width = shape[-1]
    chunks = weight_part.reshape(members, -1, width).astype(jnp.bfloat16)
    rows = chunks.shape[1]
    extra = split_in_two(norm_part).astype(jnp.bfloat16)
    packed = jnp.concatenate([chunks, jnp.broadcast_to(extra[None], (members, 8, width))], axis=1)
    arrived = lax.all_to_all(
        packed, ("row", "col"), 0, 0, tiled=True, axis_index_groups=planes
    )
    part = arrived.astype(jnp.float32).sum(axis=0)
    packed = with_split_norm(part, rows)
    arrived = lax.all_to_all(
        jnp.broadcast_to(packed[None], (half, *packed.shape)),
        "row", 0, 0, tiled=True, axis_index_groups=lines_y,
    )
    whole = arrived.astype(jnp.float32).sum(axis=0)
    chunk, sums = lax.optimization_barrier((whole[:rows].astype(jnp.bfloat16), whole[rows:]))
    weight_grad = lax.all_to_all(
        jnp.broadcast_to(chunk[None], (members, *chunk.shape)),
        ("row", "col"), 0, 0, tiled=True, axis_index_groups=planes,
    ).reshape(-1, width)
    weight_grad, norm_grad, pair_grad = final_sums(weight_grad, sums, pair_grad)
    return weight_grad.reshape(shape), norm_grad, pair_grad


def exchanged(x, axis, step):
    devices = lax.axis_size(axis)
    return lax.ppermute(x, axis, [(d, d ^ step) for d in range(devices)])


PAD = 8
VMEM_LIMIT = 24 * 2**20
ROWS_TURNED = (((1,), (1,)), ((), ()))


def turned(x):
    n = x.shape[1]
    eye = lax.broadcasted_iota(jnp.int32, (n, n), 0) == lax.broadcasted_iota(jnp.int32, (n, n), 1)
    return lax.dot_general(
        eye.astype(jnp.float32).astype(jnp.bfloat16),
        x,
        ROWS_TURNED,
        preferred_element_type=jnp.float32,
    )


def place_of():
    row, col = lax.axis_index("row"), lax.axis_index("col")
    half = lax.axis_size("row") // 2
    return lax.div(row, half), lax.rem(lax.div(col, 2), 2), lax.rem(col, 2)


def left_kernel(window_len, near_ref, far_ref, cot_ref, kept_ref, away_ref, *scratch):
    wide, by_key, product, rows_out = scratch
    hidden, cols, rows = cot_ref.shape
    x_high, _, core = place_of()
    group, step = window_len + PAD, hidden + PAD
    for source, half in ((near_ref, x_high), (far_ref, 1 - x_high)):
        for j in range(cols // 2):
            at = pl.multiple_of((half * (cols // 2) + j) * group, 8)
            wide[pl.ds(at, window_len), :] = source[pl.ds(j * window_len, window_len), :].astype(
                jnp.float32
            )
    for k in range(window_len):
        by_key[pl.ds(k * step, hidden), :] = turned(
            wide[pl.ds(k, cols, stride=group), :].astype(jnp.bfloat16)
        )
    for h in range(hidden):
        keys = by_key[pl.ds(h, window_len, stride=step), :].astype(jnp.bfloat16)
        product[pl.ds(h, window_len, stride=step), :] = jnp.dot(
            keys, cot_ref[h], preferred_element_type=jnp.float32
        )
    for k in range(window_len):
        rows_out[pl.ds(k, rows, stride=group), :] = turned(
            product[pl.ds(k * step, hidden), :].astype(jnp.bfloat16)
        )
    tokens = kept_ref.shape[1] // window_len
    for target, side in ((kept_ref, core), (away_ref, 1 - core)):
        for q in range(kept_ref.shape[0]):
            for t in range(tokens):
                at = pl.multiple_of(((2 * q + side) * tokens + t) * group, 8)
                target[q, pl.ds(t * window_len, window_len), :] = rows_out[
                    pl.ds(at, window_len), :
                ].astype(jnp.bfloat16)


def left_parts(near, far, cot_turned, blocks, window_len):
    hidden, cols, rows = cot_turned.shape
    group, step = window_len + PAD, hidden + PAD
    out = jax.ShapeDtypeStruct((blocks // 2, rows * window_len // blocks, hidden), jnp.bfloat16)
    here = pl.BlockSpec(memory_space=pltpu.VMEM)
    return pl.pallas_call(
        functools.partial(left_kernel, window_len),
        out_shape=(out, out),
        in_specs=[here, here, here],
        out_specs=(here, here),
        scratch_shapes=[
            pltpu.VMEM((cols * group, hidden), jnp.float32),
            pltpu.VMEM((window_len * step, cols), jnp.float32),
            pltpu.VMEM((window_len * step, rows), jnp.float32),
            pltpu.VMEM((rows * group, hidden), jnp.float32),
        ],
        compiler_params=pltpu.CompilerParams(vmem_limit_bytes=VMEM_LIMIT),
        name="left_parts",
    )(near, far, cot_turned)


def right_kernel(window_len, own_ref, x_ref, core_ref, both_ref, cot_ref, out_ref, *scratch):
    wide, by_key, product, rows_out = scratch
    hidden, cols, rows = cot_ref.shape
    _, x_low, core = place_of()
    group, step = window_len + PAD, hidden + PAD
    tokens = own_ref.shape[1] // window_len
    for source, x, side in (
        (own_ref, x_low, core),
        (x_ref, 1 - x_low, core),
        (core_ref, x_low, 1 - core),
        (both_ref, 1 - x_low, 1 - core),
    ):
        for z in range(own_ref.shape[0]):
            for t in range(tokens):
                at = pl.multiple_of(((z * 4 + 2 * x + side) * tokens + t) * group, 8)
                wide[pl.ds(at, window_len), :] = source[
                    z, pl.ds(t * window_len, window_len), :
                ].astype(jnp.float32)
    for k in range(window_len):
        by_key[pl.ds(k * step, hidden), :] = turned(
            wide[pl.ds(k, rows, stride=group), :].astype(jnp.bfloat16)
        )
    for h in range(hidden):
        keys = by_key[pl.ds(h, window_len, stride=step), :].astype(jnp.bfloat16)
        product[pl.ds(h, window_len, stride=step), :] = lax.dot_general(
            keys, cot_ref[h], ROWS_TURNED, preferred_element_type=jnp.float32
        )
    for k in range(window_len):
        rows_out[pl.ds(k, cols, stride=group), :] = turned(
            product[pl.ds(k * step, hidden), :].astype(jnp.bfloat16)
        )
    for j in range(cols):
        out_ref[pl.ds(j * window_len, window_len), :] = rows_out[
            pl.ds(j * group, window_len), :
        ].astype(jnp.bfloat16)


def right_parts(pieces, cot_turned, window_len):
    hidden, cols, rows = cot_turned.shape
    group, step = window_len + PAD, hidden + PAD
    here = pl.BlockSpec(memory_space=pltpu.VMEM)
    return pl.pallas_call(
        functools.partial(right_kernel, window_len),
        out_shape=jax.ShapeDtypeStruct((cols * window_len, hidden), jnp.bfloat16),
        in_specs=[here, here, here, here, here],
        out_specs=here,
        scratch_shapes=[
            pltpu.VMEM((rows * group, hidden), jnp.float32),
            pltpu.VMEM((window_len * step, rows), jnp.float32),
            pltpu.VMEM((window_len * step, cols), jnp.float32),
            pltpu.VMEM((cols * group, hidden), jnp.float32),
        ],
        compiler_params=pltpu.CompilerParams(vmem_limit_bytes=VMEM_LIMIT),
        name="right_parts",
    )(*pieces, cot_turned)


def pair_kernel(kept_ref, came_hbm, out_hbm, came, out, arrived, left):
    blocks = arrived.shape[0]
    size = kept_ref.shape[0] // blocks
    parts = [pl.ds(n * size, size) for n in range(blocks)]
    incoming = [
        pltpu.make_async_copy(came_hbm.at[part], came.at[part], arrived.at[n])
        for n, part in enumerate(parts)
    ]
    outgoing = [
        pltpu.make_async_copy(out.at[part], out_hbm.at[part], left.at[n])
        for n, part in enumerate(parts)
    ]
    for copy in incoming:
        copy.start()
    for n, part in enumerate(parts):
        incoming[n].wait()
        total = kept_ref[part].astype(jnp.float32) + came[part].astype(jnp.float32)
        out[part] = total.astype(jnp.bfloat16)
        outgoing[n].start()
    for copy in outgoing:
        copy.wait()


def pair_sum(kept, came):
    here, anywhere = pl.BlockSpec(memory_space=pltpu.VMEM), pl.BlockSpec(memory_space=pl.ANY)
    return pl.pallas_call(
        pair_kernel,
        out_shape=jax.ShapeDtypeStruct(kept.shape, kept.dtype),
        in_specs=[here, anywhere],
        out_specs=anywhere,
        scratch_shapes=[
            pltpu.VMEM(kept.shape, kept.dtype),
            pltpu.VMEM(kept.shape, kept.dtype),
            pltpu.SemaphoreType.DMA((4,)),
            pltpu.SemaphoreType.DMA((4,)),
        ],
        compiler_params=pltpu.CompilerParams(vmem_limit_bytes=VMEM_LIMIT // 4),
        name="pair_sum",
    )(kept, came)


def final_kernel(weight_ref, sums_ref, pair_ref, weight_out, norm_out, pair_out):
    pair_out[...] = pair_ref[...].astype(jnp.bfloat16)
    weight_out[...] = weight_ref[...].astype(jnp.float32)
    norm_out[...] = sums_ref[0:2, :] + sums_ref[2:4, :]


def final_sums(weight, sums, pair):
    here = pl.BlockSpec(memory_space=pltpu.VMEM)
    return pl.pallas_call(
        final_kernel,
        out_shape=(
            jax.ShapeDtypeStruct(weight.shape, jnp.float32),
            jax.ShapeDtypeStruct((2, sums.shape[1]), jnp.float32),
            jax.ShapeDtypeStruct(pair.shape, jnp.bfloat16),
        ),
        in_specs=[here, here, here],
        out_specs=(here, here, here),
        compiler_params=pltpu.CompilerParams(vmem_limit_bytes=VMEM_LIMIT // 4),
        name="final_sums",
    )(weight, sums, pair)


def all_steps(
    pair_window, tri_cotangent, saved_left, saved_right, norm_gain, norm_bias, proj_weight
):
    block_count, own_rows, col_tokens, channels = tri_cotangent.shape
    window_len = saved_left.shape[2]
    cols = lax.axis_size("col")
    rows = lax.axis_size("row")
    lines_y = [[x * (rows // 2) + y for y in range(rows // 2)] for x in range(2)]
    lines_z = [[z * 4 + k for z in range(cols // 4)] for k in range(4)]
    one_core = [[c for c in range(cols) if c % 2 == k] for k in range(2)]
    right_near = jnp.broadcast_to(saved_right, (rows // 2, *saved_right.shape[1:]))
    right_near = lax.all_to_all(
        right_near, "row", 0, 0, tiled=True, axis_index_groups=lines_y
    )
    right_far = exchanged(right_near, "row", rows // 2)
    cot_turned = lax.optimization_barrier(
        jnp.transpose(
            tri_cotangent.reshape(block_count * own_rows, col_tokens, channels), (2, 1, 0)
        )
    )
    own = jnp.broadcast_to(saved_left, (cols // 4, *saved_left.shape[1:]))
    own = lax.all_to_all(own, "col", 0, 0, tiled=True, axis_index_groups=lines_z)
    own = own.reshape(cols // 4, own_rows * window_len, channels)
    flat = (-1, channels)
    kept, away = left_parts(
        right_near.reshape(flat), right_far.reshape(flat), cot_turned, cols, window_len
    )
    came = exchanged(away, "col", 1)
    chip_part = pair_sum(kept, came)
    left_arrived = lax.all_to_all(chip_part, "col", 0, 0, tiled=True, axis_index_groups=one_core)
    across = exchanged(own, "col", 2)
    own_pair = exchanged(own, "col", 1)
    across_pair = exchanged(across, "col", 1)
    right_part = right_parts((own, across, own_pair, across_pair), cot_turned, window_len)
    right_part = right_part.reshape(col_tokens, window_len, channels)
    left_grad = left_arrived.astype(jnp.float32).sum(axis=0)
    right_grad = sent_and_summed(right_part, "row", 0)
    positions = own_rows * window_len
    pair_grad, weight_part, norm_part = gated_norm_back(
        pair_window.reshape(positions, pair_window.shape[3]),
        left_grad.reshape(positions, channels),
        right_grad.reshape(positions, channels),
        norm_gain,
        norm_bias,
        proj_weight,
    )
    pair_grad, weight_part, norm_part = lax.optimization_barrier(
        (pair_grad, weight_part, norm_part)
    )
    weight_grad, norm_grad, pair_grad = summed_over_all(weight_part, norm_part, pair_grad)
    return (pair_grad.reshape(pair_window.shape), weight_grad, norm_grad)


def solution(mesh):
    return jax.shard_map(
        all_steps,
        mesh=mesh,
        in_specs=(
            P("col", "row", None, None),
            P(None, "row", "col", None),
            P("col", "row", None, None),
            P("col", "row", None, None),
            P(),
            P(),
            P(),
        ),
        out_specs=(P("col", "row", None, None), P(), P()),
        check_vma=False,
    )
```
